32 devices in a mesh: node: 8 (over z, x), expert: 4 (over y, core).
Axes of the slice: x: 2, y: 2, z: 4, core: 2. Of those that a mesh axis runs over, the one named last changes fastest.
Arguments:
- tokens: bfloat16 [16384, 1024], P(('node', 'expert')), may hold values from -6 to 6
- queries: bfloat16 [16384, 1024], P(('node', 'expert')), may hold values from -6 to 6
- keys: bfloat16 [16384, 1024], P(('node', 'expert')), may hold values from -6 to 6
- values: bfloat16 [16384, 1024], P(('node', 'expert')), may hold values from -12 to 12
- neighbours: int32 [128, 8], P(('node', 'expert')), may hold values from 0 to 127, as said below
- live_bits: int32 [128, 8], P(('node', 'expert')), may hold values from 0 to 1, as said below
- out_proj: bfloat16 [1024, 1024], replicated, may hold values from -0.1875 to 0.1875
- norm_gain: float32 [1024], replicated, may hold values from 0.5 to 1.5
- router: bfloat16 [1024, 32], replicated, may hold values from -0.1875 to 0.1875
- expert: int32 [16384], P(('node', 'expert')), may hold values from 0 to 31, as said below
- slot: int32 [16384], P(('node', 'expert')), may hold values from 0 to 31, as said below
- w_up: bfloat16 [32, 1024, 4096], P(('node', 'expert')), may hold values from -0.1875 to 0.1875
- w_down: bfloat16 [32, 4096, 1024], P(('node', 'expert')), may hold values from -0.09375 to 0.09375
Outputs:
- layer_out: bfloat16 [16384, 1024], P(('node', 'expert'))
The draws below stay inside these ranges and needn't reach their ends.
Inputs may be any that keep to these rules, and one draw needn't show every extreme that they name: Tile g is held by device g // 4 in node-major order. neighbours[g, 0] is g itself; every listed tile is held by g's device or by the device one step before or after it along node with the same expert index (wrapping around); entry 1 is always one step before and entry 2 one step after. `live_bits`: entry 0 of every row is 1. Within the 512 tokens of one device, no two tokens share both expert and slot; some expert takes all 32 slots of every device. See expert: pairs (expert, slot) are distinct within one device's tokens.
All inputs are finite; a program needn't handle non-finite values.
Results may differ from the reference program's by a relative error of at most 0.0049.
Values may be sent and summed in bfloat16 or wider, within the bound.
A program may use at most 192 MiB of HBM per device.

```python
import jax
import jax.numpy as jnp
from jax import lax

D = 1024
HEADS = 16
HEAD_DIM = 64
FF = 4096
TILE = 128
NB = 8
TOK_DEV = 512
EXPERTS = 32
CAP = 32
TOKENS = 16384
TILES = 128
N_NODE = 8
N_EXPERT = 4
DEVICES = 32


def query_key_pair(key):
    base_query = jnp.clip(jax.random.normal(jax.random.fold_in(key, 31), (TOKENS, D), jnp.float32) * 1.3, -6.0, 6.0)
    base_key = jnp.clip(jax.random.normal(jax.random.fold_in(key, 32), (TOKENS, D), jnp.float32) * 1.3, -6.0, 6.0)
    return (base_query, base_key)


def draw_queries(key, part):
    return query_key_pair(key)[0].astype(jnp.bfloat16)


def draw_keys(key, part):
    return query_key_pair(key)[1].astype(jnp.bfloat16)


def draw_neighbours(key, part):
    tile_count = TOKENS // TILE
    tiles_dev = TOK_DEV // TILE
    tile_ids = jnp.arange(tile_count, dtype=jnp.int32)
    device_of = tile_ids // tiles_dev
    node_of = device_of // N_EXPERT
    column_of = device_of % N_EXPERT
    steps = jax.random.randint(key, (tile_count, NB), -1, 2, jnp.int32)
    steps = steps.at[:, 0].set(0).at[:, 1].set(-1).at[:, 2].set(1)
    picks = jax.random.randint(jax.random.fold_in(key, 1), (tile_count, NB), 0, tiles_dev, jnp.int32)
    other_device = (node_of[:, None] + steps + N_NODE) % N_NODE * N_EXPERT + column_of[:, None]
    listed = other_device * tiles_dev + picks
    listed = listed.at[:, 0].set(tile_ids)
    return listed.astype(jnp.int32)


def draw_live_bits(key, part):
    tile_count = TOKENS // TILE
    drawn = jax.random.randint(jax.random.fold_in(key, 5), (tile_count, NB), 0, 4, jnp.int32)
    bits = jnp.where(drawn > 0, 1, 0).astype(jnp.int32)
    return bits.at[:, 0].set(1)


def route_cells(key):
    block_count = TOKENS // TOK_DEV
    cell_count = EXPERTS * CAP
    noise = jax.random.randint(jax.random.fold_in(key, 21), (block_count, cell_count), 0, 2 ** 18, jnp.int32)
    heat = jax.random.randint(jax.random.fold_in(key, 22), (EXPERTS,), 0, 2 ** 18, jnp.int32)
    hottest = jax.random.randint(jax.random.fold_in(key, 23), (), 0, EXPERTS, jnp.int32)
    owner_of = jnp.arange(cell_count, dtype=jnp.int32) // CAP
    scores = noise + heat[owner_of][None, :] + jnp.where(owner_of == hottest, 2 ** 19, 0)[None, :]
    ranked = jnp.argsort(-scores, axis=1, stable=True)[:, :TOK_DEV]
    return ranked.reshape(TOKENS).astype(jnp.int32)


def draw_expert(key, part):
    return (route_cells(key) // CAP).astype(jnp.int32)


def draw_slot(key, part):
    return (route_cells(key) % CAP).astype(jnp.int32)


def block_scale(key, extent, split, least, top_value):
    def one(position, parts):
        draws = jax.random.uniform(jax.random.fold_in(jax.random.fold_in(key, 6), position), (parts,), jnp.float32, least / len(split), top_value / len(split))
        return jnp.repeat(jnp.exp(draws), extent[position] // parts).reshape((-1,) + (1,) * (len(extent) - position - 1))

    loudness = one(*split[0])
    for cut in split[1:]:
        loudness = loudness * one(*cut)
    return loudness


def scatter_about(rng, extent, deviation, bound, pieces=(), held_as=jnp.bfloat16):
    values = jax.random.normal(rng, extent, jnp.float32) * deviation
    if len(pieces) > 0:
        values = block_scale(rng, extent, pieces, -0.22, 0.18) * values
    return jnp.clip(values, min=-bound, max=bound).astype(held_as)


def setup_inputs(seed: int = 0) -> dict:
    seeds = jax.random.split(jax.random.key(seed), 14)
    tokens = scatter_about(seeds[0], (TOKENS, D), 1.0, 6.0, ((0, 32),))
    queries = draw_queries(jax.random.fold_in(seeds[13], 71), 0)
    keys = draw_keys(jax.random.fold_in(seeds[13], 71), 0)
    values = scatter_about(seeds[3], (TOKENS, D), 2.0, 12.0, ((0, 32),))
    neighbours = draw_neighbours(jax.random.fold_in(seeds[13], 71), 0)
    live_bits = draw_live_bits(jax.random.fold_in(seeds[13], 71), 0)
    out_proj = scatter_about(seeds[6], (D, D), D ** -0.5, 0.1875)
    norm_gain = jnp.clip(1.0 + 0.1 * jax.random.normal(seeds[7], (D,), jnp.float32), 0.5, 1.5)
    router = scatter_about(seeds[8], (D, EXPERTS), D ** -0.5, 0.1875)
    expert = draw_expert(jax.random.fold_in(seeds[13], 71), 0)
    slot = draw_slot(jax.random.fold_in(seeds[13], 71), 0)
    w_up = scatter_about(seeds[11], (EXPERTS, D, FF), D ** -0.5, 0.1875, ((0, 32),))
    w_down = scatter_about(seeds[12], (EXPERTS, FF, D), FF ** -0.5, 0.09375, ((0, 32),))
    return dict(tokens=tokens, queries=queries, keys=keys, values=values, neighbours=neighbours, live_bits=live_bits, out_proj=out_proj, norm_gain=norm_gain, router=router, expert=expert, slot=slot, w_up=w_up, w_down=w_down)


score_scale = 0.125

def attend_tile(packed, key_tiles, value_tiles):
    query_tile, listed, bits = packed
    near_keys = key_tiles[listed].reshape(NB * TILE, HEADS, HEAD_DIM).astype(jnp.float32)
    near_values = value_tiles[listed].reshape(NB * TILE, HEADS, HEAD_DIM).astype(jnp.float32)
    query_heads = query_tile.reshape(TILE, HEADS, HEAD_DIM).astype(jnp.float32)
    scores = jnp.einsum('qhd,khd->hqk', query_heads, near_keys) * score_scale
    visible = jnp.repeat(bits, TILE) > 0
    masked = jnp.where(visible[None, None, :], scores, -jnp.inf)
    peak = lax.optimization_barrier(jnp.max(masked, axis=-1, keepdims=True))
    weights = jnp.exp(masked - peak)
    weights = (weights / lax.optimization_barrier(jnp.sum(weights, axis=-1, keepdims=True))).astype(jnp.bfloat16)
    mixed = jnp.einsum('hqk,khd->qhd', weights.astype(jnp.float32), near_values)
    return mixed.reshape(TILE, D).astype(jnp.bfloat16)

def reference(tokens, queries, keys, values, neighbours, live_bits, out_proj, norm_gain, router, expert, slot, w_up, w_down):
    key_tiles = keys.reshape(TILES, TILE, D)
    value_tiles = values.reshape(TILES, TILE, D)
    query_tiles = queries.reshape(TILES, TILE, D)
    attn = lax.map(lambda packed: attend_tile(packed, key_tiles, value_tiles), (query_tiles, neighbours, live_bits))
    attn = attn.reshape(TOKENS, D)
    hidden = tokens.astype(jnp.float32) + jnp.dot(attn, out_proj, preferred_element_type=jnp.float32)
    spread = lax.optimization_barrier(jnp.mean(hidden * hidden, axis=-1, keepdims=True))
    normed = (hidden * lax.rsqrt(spread + 1e-06) * norm_gain.astype(jnp.float32)[None, :]).astype(jnp.bfloat16)
    logits = jnp.dot(normed, router, preferred_element_type=jnp.float32)
    columns = jnp.arange(EXPERTS, dtype=jnp.int32)
    chosen = lax.optimization_barrier(jnp.sum(jnp.where(columns[None, :] == expert[:, None], logits, 0.0), axis=-1))
    gate = jax.nn.sigmoid(chosen)
    positions = jnp.arange(TOKENS, dtype=jnp.int32)
    target = expert * (DEVICES * CAP) + positions // TOK_DEV * CAP + slot
    table = jnp.full((EXPERTS * DEVICES * CAP,), TOKENS, jnp.int32).at[target].set(positions)
    padded = jnp.concatenate([normed, jnp.zeros((1, D), jnp.bfloat16)], axis=0)

    def run_expert(packed):
        index_rows, up_matrix, down_matrix = packed
        token_rows = padded[index_rows]
        lifted = jnp.dot(token_rows, up_matrix, preferred_element_type=jnp.float32)
        lifted = jax.nn.gelu(lifted, approximate=True).astype(jnp.bfloat16)
        return jnp.dot(lifted, down_matrix, preferred_element_type=jnp.float32).astype(jnp.bfloat16)
    results = lax.map(run_expert, (table.reshape(EXPERTS, DEVICES * CAP), w_up, w_down))
    expert_out = results.reshape(EXPERTS * DEVICES * CAP, D)[target]
    layer_out = hidden + gate[:, None] * expert_out.astype(jnp.float32)
    return layer_out.astype(jnp.bfloat16)
```

```python
import functools

import jax
import jax.numpy as jnp
from jax import lax
from jax.experimental import pallas as pl
from jax.experimental.pallas import tpu as pltpu
from jax.sharding import PartitionSpec as P

D = 1024
HEADS = 16
HEAD_DIM = 64
TILE = 128
NB = 8


score_scale = 0.125


LANES = 128
HIDE = -1e30


def attention_kernel(
    nodes,
    columns,
    neighbour_ref,
    live_ref,
    query_hbm,
    key_ref,
    value_ref,
    token_hbm,
    proj_hbm,
    router_ref,
    gain_ref,
    expert_ref,
    hidden_ref,
    normed_ref,
    gate_ref,
    level_ref,
    *scratch,
):
    chunks = D // LANES
    key_windows, value_windows = scratch[:chunks], scratch[chunks : 2 * chunks]
    own_sem, x_send, x_recv, z_send, z_recv, attn_ref = scratch[2 * chunks : 2 * chunks + 6]
    query_ref, token_ref, proj_ref, load_sem = scratch[2 * chunks + 6 : 2 * chunks + 10]
    bias_ref, weight_ref, count_ref, peers_ref, level_send, level_recv = scratch[2 * chunks + 10 :]
    devices = nodes * columns
    token_load = pltpu.make_async_copy(token_hbm, token_ref, load_sem.at[0])
    proj_load = pltpu.make_async_copy(proj_hbm, proj_ref, load_sem.at[1])
    query_load = pltpu.make_async_copy(query_hbm, query_ref, load_sem.at[2])
    node = lax.axis_index("node")
    me = node * columns + lax.axis_index("expert")
    odd = node % 2
    partner = node + 1 - 2 * odd
    onward = (node + 2 - 4 * odd + nodes) % nodes
    tiles = key_windows[0].shape[0] // 3
    barrier = pltpu.get_barrier_semaphore()

    def place(device):
        return {"node": device // columns, "expert": device % columns}

    def greet(k, carry):
        pl.semaphore_signal(
            barrier,
            inc=1,
            device_id=place((me + k) % devices),
            device_id_type=pl.DeviceIdType.MESH,
        )
        return carry

    lax.fori_loop(1, devices, greet, 0)

    members = devices // GROUPS
    plane = me // members
    away = (expert_ref[...] // members - plane + GROUPS) % GROUPS
    most = jnp.zeros((1, 1), jnp.float32)
    for g in range(1, GROUPS):
        most = jnp.maximum(
            most, jnp.sum(jnp.where(away == g, 1.0, 0.0), axis=1, keepdims=True)
        )
    count_ref[...] = jnp.broadcast_to(most, count_ref.shape)
    peers_ref[me] = jnp.broadcast_to(most, count_ref.shape)

    own, first, second = [], [], []
    for c in range(chunks):
        lanes = pl.ds(c * LANES, LANES)
        for s, (source, window) in enumerate(
            ((key_ref, key_windows[c]), (value_ref, value_windows[c]))
        ):
            block = source.at[:, :, lanes]
            own.append(
                pltpu.make_async_copy(block, window.at[pl.ds(0, tiles)], own_sem.at[2 * c + s])
            )
            first.append(
                pltpu.make_async_remote_copy(
                    src_ref=block,
                    dst_ref=window.at[pl.ds(tiles, tiles)],
                    send_sem=x_send.at[2 * c + s],
                    recv_sem=x_recv.at[2 * c + s],
                    device_id={"node": partner},
                    device_id_type=pl.DeviceIdType.MESH,
                )
            )
            second.append(
                pltpu.make_async_remote_copy(
                    src_ref=window.at[pl.ds(tiles, tiles)],
                    dst_ref=window.at[pl.ds(2 * tiles, tiles)],
                    send_sem=z_send.at[2 * c + s],
                    recv_sem=z_recv.at[2 * c + s],
                    device_id={"node": onward},
                    device_id_type=pl.DeviceIdType.MESH,
                )
            )

    def tell(k, source):
        return pltpu.make_async_remote_copy(
            src_ref=count_ref,
            dst_ref=peers_ref.at[source],
            send_sem=level_send.at[k],
            recv_sem=level_recv.at[k],
            device_id=place((me + k) % devices),
            device_id_type=pl.DeviceIdType.MESH,
        )

    def each_peer(act):
        def step(k, carry):
            act(k)
            return carry

        lax.fori_loop(1, devices, step, 0)

    pl.semaphore_wait(barrier, devices - 1)
    for copy in first:
        copy.start()
    for copy in own + [token_load, query_load, proj_load]:
        copy.start()
    each_peer(lambda k: tell(k, me).start())
    for t in range(tiles):
        for j in range(NB):
            hide = jnp.where(live_ref[t, j] > 0, 0.0, HIDE)
            bias_ref[t, j * TILE : (j + 1) * TILE, :] = jnp.full(
                (TILE, LANES), hide, jnp.float32
            ).astype(jnp.bfloat16)
    token_load.wait()
    hidden_ref[...] = token_ref[...].astype(jnp.float32)
    lane = lax.broadcasted_iota(jnp.int32, (TILE, LANES), 1)
    low = lane < HEAD_DIM
    mark = (lax.broadcasted_iota(jnp.int32, (2 * TILE, LANES), 1) == 0).astype(jnp.bfloat16)
    ones = jnp.ones((NB * TILE, LANES), jnp.bfloat16)

    def position(t, j):
        listed = neighbour_ref[t, j]
        owner = listed // (tiles * columns)
        block = jnp.where(owner == node, 0, jnp.where(owner == partner, 1, 2))
        return block * tiles + listed % tiles

    def scores_of(c, t):
        query = query_ref[t * TILE : (t + 1) * TILE, c * LANES : (c + 1) * LANES]
        query = query * jnp.bfloat16(score_scale)
        blank = jnp.zeros_like(query)
        mine = jnp.concatenate(
            [jnp.where(low, query, blank), jnp.where(low, blank, query)], axis=0
        )
        near_keys = jnp.concatenate(
            [key_windows[c][position(t, j)] for j in range(NB)], axis=0
        )
        scores = lax.dot_general(
            jnp.concatenate([mine, mark], axis=1),
            jnp.concatenate([near_keys, bias_ref[t]], axis=1),
            (((1,), (1,)), ((), ())),
            preferred_element_type=jnp.float32,
        )
        peak = jnp.max(scores, axis=-1, keepdims=True)
        weight_ref[t] = jnp.exp(scores - peak).astype(jnp.bfloat16)

    def values_of(c, t):
        near_values = jnp.concatenate(
            [value_windows[c][position(t, j)] for j in range(NB)], axis=0
        )
        out = jnp.dot(
            weight_ref[t],
            jnp.concatenate([near_values, ones], axis=1),
            preferred_element_type=jnp.float32,
        )
        share = out[:, :LANES] / out[:, LANES:]
        attn_ref[t * TILE : (t + 1) * TILE, :] = jnp.where(
            low, share[:TILE], share[TILE:]
        ).astype(jnp.bfloat16)

    def relay(i):
        if i < 2 * chunks:
            first[i].wait_recv()
            second[i].start()

    query_load.wait()
    proj_load.wait()
    relay(0)
    for c in range(chunks):
        relay(2 * c + 1)
        own[2 * c].wait()
        second[2 * c].wait_recv()
        for t in range(tiles):
            scores_of(c, t)
        relay(2 * c + 2)
        own[2 * c + 1].wait()
        if c == chunks - 1:
            each_peer(lambda k: tell(k, (me - k + devices) % devices).wait_recv())
            level_ref[...] = jnp.max(peers_ref[...], axis=0)
            for copy in first:
                copy.wait_send()
            each_peer(lambda k: tell(k, me).wait_send())
        second[2 * c + 1].wait_recv()
        for t in range(tiles):
            values_of(c, t)
        hidden_ref[...] += jnp.dot(
            attn_ref[...],
            proj_ref[c * LANES : (c + 1) * LANES, :],
            preferred_element_type=jnp.float32,
        )

    def finish(t, carry):
        rows = pl.ds(pl.multiple_of(t * TILE, TILE), TILE)
        hidden = hidden_ref[rows, :]
        spread = jnp.mean(hidden * hidden, axis=-1, keepdims=True)
        normed = (hidden * lax.rsqrt(spread + 1e-06) * gain_ref[...]).astype(jnp.bfloat16)
        normed_ref[rows, :] = normed
        logits = jnp.dot(normed, router_ref[...], preferred_element_type=jnp.float32)
        experts = logits.shape[1]
        wanted = jnp.transpose(
            jnp.broadcast_to(expert_ref[:, rows].astype(jnp.float32), (TILE, TILE))
        )[:, :experts]
        column = lax.broadcasted_iota(jnp.int32, (TILE, experts), 1).astype(jnp.float32)
        chosen = jnp.sum(jnp.where(wanted == column, logits, 0.0), axis=-1, keepdims=True)
        gate_ref[rows, :] = jnp.broadcast_to(jax.nn.sigmoid(chosen), (TILE, LANES))
        return carry

    lax.fori_loop(0, tiles, finish, 0)
    for copy in second:
        copy.wait_send()


def attention_block(
    tokens, queries, keys, values, neighbours, live_bits, out_proj, norm_gain, router, expert
):
    tok_dev = tokens.shape[0]
    tiles = tok_dev // TILE
    chunks = D // LANES
    devices = lax.axis_size("node") * lax.axis_size("expert")
    window = pltpu.VMEM((3 * tiles, TILE, LANES), jnp.bfloat16)
    sems = pltpu.SemaphoreType.DMA((2 * chunks,))
    vmem = pl.BlockSpec(memory_space=pltpu.VMEM)
    smem = pl.BlockSpec(memory_space=pltpu.SMEM)
    anywhere = pl.BlockSpec(memory_space=pl.ANY)
    return pl.pallas_call(
        functools.partial(attention_kernel, lax.axis_size("node"), lax.axis_size("expert")),
        out_shape=(
            jax.ShapeDtypeStruct((tok_dev, D), jnp.float32),
            jax.ShapeDtypeStruct((tok_dev, D), jnp.bfloat16),
            jax.ShapeDtypeStruct((tok_dev, LANES), jnp.float32),
            jax.ShapeDtypeStruct((8, LANES), jnp.float32),
        ),
        in_specs=[smem, smem] + [anywhere] * 5 + [vmem] * 3,
        out_specs=(vmem,) * 4,
        scratch_shapes=[window] * (2 * chunks)
        + [sems] * 5
        + [
            pltpu.VMEM((tok_dev, LANES), jnp.bfloat16),
            pltpu.VMEM((tok_dev, D), jnp.bfloat16),
            pltpu.VMEM((tok_dev, D), jnp.bfloat16),
            pltpu.VMEM((D, D), jnp.bfloat16),
            pltpu.SemaphoreType.DMA((3,)),
            pltpu.VMEM((tiles, NB * TILE, LANES), jnp.bfloat16),
            pltpu.VMEM((tiles, 2 * TILE, NB * TILE), jnp.bfloat16),
            pltpu.VMEM((8, LANES), jnp.float32),
            pltpu.VMEM((devices, 8, LANES), jnp.float32),
            pltpu.SemaphoreType.DMA((devices,)),
            pltpu.SemaphoreType.DMA((devices,)),
        ],
        compiler_params=pltpu.CompilerParams(
            collective_id=0, has_side_effects=True, vmem_limit_bytes=62 * 1024 * 1024
        ),
    )(
        neighbours,
        live_bits,
        queries,
        keys.reshape(tiles, TILE, D),
        values.reshape(tiles, TILE, D),
        tokens,
        out_proj,
        router,
        norm_gain.reshape(1, D),
        expert.reshape(1, tok_dev),
    )


GROUPS = 4
SPAN = 512
ORDER = (2, 1, 3)


def expert_kernel(
    nodes, columns, outgoing_ref, up_ref, down_ref, back_ref, *scratch
):
    (
        rows_ref,
        result_ref,
        up_held,
        down_held,
        total_ref,
        weight_sem,
        own_sem,
        there_send,
        there_recv,
        back_send,
        back_recv,
    ) = scratch
    devices = nodes * columns
    cap = outgoing_ref.shape[1]
    members = devices // GROUPS
    me = lax.axis_index("node") * columns + lax.axis_index("expert")
    up_copy = pltpu.make_async_copy(up_ref.at[0], up_held, weight_sem.at[0])
    down_copy = pltpu.make_async_copy(down_ref.at[0], down_held, weight_sem.at[1])

    def place(device):
        return {"node": device // columns, "expert": device % columns}

    barrier = pltpu.get_barrier_semaphore()

    def greet(k, carry):
        pl.semaphore_signal(
            barrier,
            inc=1,
            device_id=place((me + k) % devices),
            device_id_type=pl.DeviceIdType.MESH,
        )
        return carry

    lax.fori_loop(1, devices, greet, 0)
    pl.semaphore_wait(barrier, devices - 1)

    def block(g, j):
        return pl.ds(pl.multiple_of(j * cap, cap), cap)

    def there(i):
        g, j = i // members, i % members
        target = (me + g + GROUPS * j) % devices
        return pltpu.make_async_remote_copy(
            src_ref=outgoing_ref.at[target],
            dst_ref=rows_ref.at[g, block(g, j)],
            send_sem=there_send.at[i],
            recv_sem=there_recv.at[i],
            device_id=place(target),
            device_id_type=pl.DeviceIdType.MESH,
        )

    def back(i):
        g, j = i // members, i % members
        target = (me + devices - g - GROUPS * j) % devices
        return pltpu.make_async_remote_copy(
            src_ref=result_ref.at[g, block(g, j)],
            dst_ref=back_ref.at[me],
            send_sem=back_send.at[i],
            recv_sem=back_recv.at[i],
            device_id=place(target),
            device_id_type=pl.DeviceIdType.MESH,
        )

    def back_from(i):
        g, j = i // members, i % members
        source = (me + g + GROUPS * j) % devices
        return pltpu.make_async_remote_copy(
            src_ref=result_ref.at[g, block(g, j)],
            dst_ref=back_ref.at[source],
            send_sem=back_send.at[i],
            recv_sem=back_recv.at[i],
            device_id=place(source),
            device_id_type=pl.DeviceIdType.MESH,
        )

    def each(lower, upper, act):
        def step(i, carry):
            act(i)
            return carry

        lax.fori_loop(lower, upper, step, 0)

    each(1, devices, lambda i: there(i).start())
    up_copy.start()
    down_copy.start()
    own_rows = pltpu.make_async_copy(
        outgoing_ref.at[me], rows_ref.at[0, pl.ds(0, cap)], own_sem.at[0]
    )
    own_rows.start()
    own_back = pltpu.make_async_copy(
        result_ref.at[0, pl.ds(0, cap)], back_ref.at[me], own_sem.at[1]
    )
    spans = up_held.shape[1] // SPAN
    for g in range(GROUPS):
        first = max(g * members, 1)
        each(first, (g + 1) * members, lambda i: there(i).wait_recv())
        if g == 0:
            own_rows.wait()
            up_copy.wait()
            down_copy.wait()

        def span(f, carry, g=g):
            part = pl.ds(pl.multiple_of(f * SPAN, SPAN), SPAN)
            lifted = jnp.dot(rows_ref[g], up_held[:, part], preferred_element_type=jnp.float32)
            lifted = jax.nn.gelu(lifted, approximate=True).astype(jnp.bfloat16)
            total_ref[...] += jnp.dot(
                lifted, down_held[part, :], preferred_element_type=jnp.float32
            )
            return carry

        total_ref[...] = jnp.zeros_like(total_ref)
        lax.fori_loop(0, spans, span, 0)
        result_ref[g] = total_ref[...].astype(jnp.bfloat16)
        if g == 0:
            own_back.start()
        each(first, (g + 1) * members, lambda i: back(i).start())
    own_back.wait()
    each(1, devices, lambda i: there(i).wait_send())
    each(1, devices, lambda i: back(i).wait_send())
    each(1, devices, lambda i: back_from(i).wait_recv())


def expert_exchange(outgoing, w_up, w_down):
    devices, cap, _ = outgoing.shape
    hidden_units = w_up.shape[2]
    rows = devices // GROUPS * cap
    anywhere = pl.BlockSpec(memory_space=pl.ANY)
    sems = pltpu.SemaphoreType.DMA((devices,))
    pair = pltpu.SemaphoreType.DMA((2,))
    return pl.pallas_call(
        functools.partial(expert_kernel, lax.axis_size("node"), lax.axis_size("expert")),
        out_shape=jax.ShapeDtypeStruct(outgoing.shape, jnp.bfloat16),
        in_specs=[anywhere] * 3,
        out_specs=anywhere,
        scratch_shapes=[
            pltpu.VMEM((GROUPS, rows, D), jnp.bfloat16),
            pltpu.VMEM((GROUPS, rows, D), jnp.bfloat16),
            pltpu.VMEM((D, hidden_units), jnp.bfloat16),
            pltpu.VMEM((hidden_units, D), jnp.bfloat16),
            pltpu.VMEM((rows, D), jnp.float32),
            pair,
            pair,
            sems,
            sems,
            sems,
            sems,
        ],
        compiler_params=pltpu.CompilerParams(
            collective_id=1, has_side_effects=True, vmem_limit_bytes=62 * 1024 * 1024
        ),
    )(outgoing, w_up, w_down)


def relay_kernel(
    nodes,
    columns,
    normed_ref,
    hidden_hbm,
    gate_ref,
    expert_ref,
    slot_ref,
    up_ref,
    down_ref,
    out_ref,
    up_held,
    down_held,
    hidden_ref,
    total_ref,
    mixed_ref,
    packed_ref,
    guide_ref,
    taken_ref,
    taken_guide_ref,
    padded_ref,
    rows_ref,
    result_ref,
    back_ref,
    repacked_ref,
    home_ref,
    load_sem,
    hop_send,
    hop_recv,
    guide_send,
    guide_recv,
    home_send,
    home_recv,
    there_send,
    there_recv,
    back_send,
    back_recv,
):
    devices = nodes * columns
    members = devices // GROUPS
    tok_dev = normed_ref.shape[0]
    fit = packed_ref.shape[1]
    block = rows_ref.shape[1] // members
    cells = members * block
    me = lax.axis_index("node") * columns + lax.axis_index("expert")
    plane, member = me // members, me % members
    up_copy = pltpu.make_async_copy(up_ref.at[0], up_held, load_sem.at[0])
    down_copy = pltpu.make_async_copy(down_ref.at[0], down_held, load_sem.at[1])
    hidden_copy = pltpu.make_async_copy(hidden_hbm, hidden_ref, load_sem.at[2])

    def place(device):
        return {"node": device // columns, "expert": device % columns}

    def mate(g):
        return place((plane + g) % GROUPS * members + member)

    def peer(k):
        return place(plane * members + (member + k) % members)

    barrier = pltpu.get_barrier_semaphore()
    for target in [mate(g) for g in range(1, GROUPS)] + [peer(k) for k in range(1, members)]:
        pl.semaphore_signal(
            barrier, inc=1, device_id=target, device_id_type=pl.DeviceIdType.MESH
        )
    up_copy.start()
    down_copy.start()
    hidden_copy.start()

    away = (expert_ref[...] // members - plane + GROUPS) % GROUPS
    cell = expert_ref[...] % members * block + slot_ref[...]
    lines = lax.broadcasted_iota(jnp.int32, (8, tok_dev), 0)
    earlier = (
        lax.broadcasted_iota(jnp.int32, (tok_dev, tok_dev), 0)
        < lax.broadcasted_iota(jnp.int32, (tok_dev, tok_dev), 1)
    ).astype(jnp.bfloat16)
    ranks = jnp.dot(
        (lines == away).astype(jnp.bfloat16), earlier, preferred_element_type=jnp.float32
    ).astype(jnp.int32)
    cell_lines = jnp.broadcast_to((cell + 1).astype(jnp.float32), (8, tok_dev)).astype(
        jnp.bfloat16
    )
    seats = [jnp.where(away == 0, cell, -1)] + [
        jnp.where(away == g, ranks[g : g + 1, :], -1) for g in range(1, GROUPS)
    ]

    def spread(g, count):
        return (lax.broadcasted_iota(jnp.int32, (count, tok_dev), 0) == seats[g]).astype(
            jnp.bfloat16
        )

    def hop(g):
        return pltpu.make_async_remote_copy(
            src_ref=packed_ref.at[g - 1],
            dst_ref=taken_ref.at[g - 1],
            send_sem=hop_send.at[g],
            recv_sem=hop_recv.at[g],
            device_id=mate(g),
            device_id_type=pl.DeviceIdType.MESH,
        )

    def guide(g):
        return pltpu.make_async_remote_copy(
            src_ref=guide_ref.at[g - 1],
            dst_ref=taken_guide_ref.at[g - 1],
            send_sem=guide_send.at[g],
            recv_sem=guide_recv.at[g],
            device_id=mate(g),
            device_id_type=pl.DeviceIdType.MESH,
        )

    def homeward(g):
        return pltpu.make_async_remote_copy(
            src_ref=repacked_ref.at[g - 1],
            dst_ref=home_ref.at[g - 1],
            send_sem=home_send.at[g],
            recv_sem=home_recv.at[g],
            device_id=mate(GROUPS - g),
            device_id_type=pl.DeviceIdType.MESH,
        )

    def part(k):
        return pl.ds(pl.multiple_of(k % members * block, block), block)

    def there(g, k, source):
        return pltpu.make_async_remote_copy(
            src_ref=padded_ref.at[g, part(member + k)],
            dst_ref=rows_ref.at[g, part(source)],
            send_sem=there_send.at[g, k],
            recv_sem=there_recv.at[g, k],
            device_id=peer(k),
            device_id_type=pl.DeviceIdType.MESH,
        )

    def back(g, k, source):
        return pltpu.make_async_remote_copy(
            src_ref=result_ref.at[g, part(member + k)],
            dst_ref=back_ref.at[g, part(source)],
            send_sem=back_send.at[g, k],
            recv_sem=back_recv.at[g, k],
            device_id=peer(k),
            device_id_type=pl.DeviceIdType.MESH,
        )

    def each(act):
        def step(k, carry):
            act(k)
            return carry

        lax.fori_loop(1, members, step, 0)

    def hand_out(g):
        each(lambda k: there(g, k, member).start())
        rows_ref[g, part(member), :] = padded_ref[g, part(member), :]

    def placing(g):
        return (
            lax.broadcasted_iota(jnp.int32, (cells, fit), 0).astype(jnp.float32) + 1.0
            == taken_guide_ref[g - 1, 0:1, :]
        ).astype(jnp.bfloat16)

    def expand(g):
        guide(g).wait_recv()
        hop(g).wait_recv()
        padded_ref[g] = jnp.dot(
            placing(g), taken_ref[g - 1], preferred_element_type=jnp.float32
        ).astype(jnp.bfloat16)
        hand_out(g)

    def compute(g):
        each(lambda k: there(g, k, member + members - k).wait_recv())

        def span(f, carry):
            columns_f = pl.ds(pl.multiple_of(f * SPAN, SPAN), SPAN)
            lifted = jnp.dot(
                rows_ref[g], up_held[:, columns_f], preferred_element_type=jnp.float32
            )
            lifted = jax.nn.gelu(lifted, approximate=True).astype(jnp.bfloat16)
            total_ref[...] += jnp.dot(
                lifted, down_held[columns_f, :], preferred_element_type=jnp.float32
            )
            return carry

        total_ref[...] = jnp.zeros_like(total_ref)
        lax.fori_loop(0, up_held.shape[1] // SPAN, span, 0)
        result_ref[g] = total_ref[...].astype(jnp.bfloat16)
        each(lambda k: back(g, k, member).start())
        back_ref[g, part(member), :] = result_ref[g, part(member), :]

    def collect(g):
        each(lambda k: back(g, k, member + members - k).wait_recv())

    def repack(g):
        collect(g)
        repacked_ref[g - 1] = lax.dot_general(
            placing(g),
            back_ref[g],
            (((0,), (0,)), ((), ())),
            preferred_element_type=jnp.float32,
        ).astype(jnp.bfloat16)
        homeward(g).start()

    def take_home(g, source, count):
        seated = spread(g, count)
        return lax.dot_general(
            seated, source, (((0,), (0,)), ((), ())), preferred_element_type=jnp.float32
        )

    for g in ORDER:
        seated = spread(g, fit)
        packed_ref[g - 1] = jnp.dot(
            seated, normed_ref[...], preferred_element_type=jnp.float32
        ).astype(jnp.bfloat16)
        guide_ref[g - 1] = lax.dot_general(
            cell_lines, seated, (((1,), (1,)), ((), ())), preferred_element_type=jnp.float32
        )
        if g == ORDER[0]:
            pl.semaphore_wait(barrier, GROUPS + members - 2)
        guide(g).start()
        hop(g).start()
    padded_ref[0] = jnp.dot(
        spread(0, cells), normed_ref[...], preferred_element_type=jnp.float32
    ).astype(jnp.bfloat16)
    hand_out(0)
    up_copy.wait()
    down_copy.wait()
    compute(0)
    one, two, three = ORDER
    expand(one)
    collect(0)
    mixed_ref[...] = take_home(0, back_ref[0], cells)
    expand(two)
    compute(one)
    compute(two)
    expand(three)
    repack(one)
    repack(two)
    compute(three)
    repack(three)
    hidden_copy.wait()
    for g in ORDER[:-1]:
        homeward(g).wait_recv()
        mixed_ref[...] += take_home(g, home_ref[g - 1], fit)
    homeward(three).wait_recv()
    mixed = mixed_ref[...] + take_home(three, home_ref[three - 1], fit)
    out_ref[...] = (hidden_ref[...] + gate_ref[:, 0:1] * mixed).astype(jnp.bfloat16)
    for g in range(GROUPS):
        each(lambda k: there(g, k, member).wait_send())
        each(lambda k: back(g, k, member).wait_send())
    for g in ORDER:
        guide(g).wait_send()
        hop(g).wait_send()
        homeward(g).wait_send()


def relay_exchange(fit, normed, hidden, gate, expert, slot, w_up, w_down):
    tok_dev = normed.shape[0]
    hidden_units = w_up.shape[2]
    nodes, columns = lax.axis_size("node"), lax.axis_size("expert")
    members = nodes * columns // GROUPS
    cells = 2 * tok_dev // GROUPS
    anywhere = pl.BlockSpec(memory_space=pl.ANY)
    vmem = pl.BlockSpec(memory_space=pltpu.VMEM)
    packed = pltpu.VMEM((GROUPS - 1, fit, D), jnp.bfloat16)
    guides = pltpu.VMEM((GROUPS - 1, 8, fit), jnp.float32)
    grouped = pltpu.VMEM((GROUPS, cells, D), jnp.bfloat16)
    hop_sems = pltpu.SemaphoreType.DMA((GROUPS,))
    peer_sems = pltpu.SemaphoreType.DMA((GROUPS, members))
    return pl.pallas_call(
        functools.partial(relay_kernel, nodes, columns),
        out_shape=jax.ShapeDtypeStruct((tok_dev, D), jnp.bfloat16),
        in_specs=[vmem, anywhere, vmem, vmem, vmem, anywhere, anywhere],
        out_specs=vmem,
        scratch_shapes=[
            pltpu.VMEM((D, hidden_units), jnp.bfloat16),
            pltpu.VMEM((hidden_units, D), jnp.bfloat16),
            pltpu.VMEM((tok_dev, D), jnp.float32),
            pltpu.VMEM((cells, D), jnp.float32),
            pltpu.VMEM((tok_dev, D), jnp.float32),
            packed,
            guides,
            packed,
            guides,
            grouped,
            grouped,
            grouped,
            grouped,
            packed,
            packed,
            pltpu.SemaphoreType.DMA((3,)),
        ]
        + [hop_sems] * 6
        + [peer_sems] * 4,
        compiler_params=pltpu.CompilerParams(
            collective_id=2, has_side_effects=True, vmem_limit_bytes=62 * 1024 * 1024
        ),
    )(
        normed,
        hidden,
        gate,
        expert.reshape(1, tok_dev),
        slot.reshape(1, tok_dev),
        w_up,
        w_down,
    )


def exchange_by_blocks(outgoing, w_up, w_down):
    experts, cap, _ = outgoing.shape
    block = lax.all_to_all(
        outgoing.reshape(experts, 1, cap, D),
        ("node", "expert"),
        split_axis=0,
        concat_axis=1,
        tiled=True,
    )
    token_rows = block.reshape(-1, D)
    lifted = jnp.dot(token_rows, w_up[0], preferred_element_type=jnp.float32)
    lifted = jax.nn.gelu(lifted, approximate=True).astype(jnp.bfloat16)
    result = jnp.dot(lifted, w_down[0], preferred_element_type=jnp.float32).astype(jnp.bfloat16)
    return lax.all_to_all(
        result.reshape(block.shape), ("node", "expert"), split_axis=1, concat_axis=0, tiled=True
    )


def shards(
    tokens,
    queries,
    keys,
    values,
    neighbours,
    live_bits,
    out_proj,
    norm_gain,
    router,
    expert,
    slot,
    w_up,
    w_down,
):
    tok_dev = tokens.shape[0]
    experts = router.shape[1]
    cap = 2 * tok_dev // experts
    hidden, normed, gate, level = attention_block(
        tokens, queries, keys, values, neighbours, live_bits, out_proj, norm_gain, router, expert
    )

    def padded_way():
        slot_cell = expert * cap + slot
        one_hot = (lax.iota(jnp.int32, experts * cap)[:, None] == slot_cell[None, :]).astype(
            jnp.bfloat16
        )
        outgoing = jnp.dot(one_hot, normed, preferred_element_type=jnp.float32).astype(
            jnp.bfloat16
        )
        exchange = exchange_by_blocks if cap % 16 else expert_exchange
        returned = exchange(outgoing.reshape(experts, cap, D), w_up, w_down)
        flat_back = returned.reshape(experts * cap, D)
        expert_out = jnp.einsum(
            "ct,cd->td", one_hot, flat_back, preferred_element_type=jnp.float32
        )
        layer_out = hidden + gate[:, :1] * expert_out
        return layer_out.astype(jnp.bfloat16)

    def relayed_way():
        return relay_exchange(fit, normed, hidden, gate, expert, slot, w_up, w_down)

    fit = 2 * tok_dev // GROUPS * 3 // 4
    if cap % 16 or lax.axis_size("node") % GROUPS:
        return padded_way()
    return lax.cond(level[0, 0] <= fit, relayed_way, padded_way)


def solution(mesh):
    in_specs = (
        P(("node", "expert"), None),
        P(("node", "expert"), None),
        P(("node", "expert"), None),
        P(("node", "expert"), None),
        P(("node", "expert"), None),
        P(("node", "expert"), None),
        P(),
        P(),
        P(),
        P(("node", "expert")),
        P(("node", "expert")),
        P(("node", "expert"), None, None),
        P(("node", "expert"), None, None),
    )
    out_specs = P(("node", "expert"), None)
    return jax.shard_map(shards, mesh=mesh, in_specs=in_specs, out_specs=out_specs, check_vma=False)
```

```python
import functools

import jax
import jax.numpy as jnp
from jax import lax
from jax.experimental import pallas as pl
from jax.experimental.pallas import tpu as pltpu
from jax.sharding import PartitionSpec as P

D = 1024
HEADS = 16
HEAD_DIM = 64
TILE = 128
NB = 8


score_scale = 0.125


LANES = 128
GROUPS = 4
RELAYED = (2, 3)


def across(plane, g):
    if g % 2:
        plane = plane + 1 - 2 * (plane % 2)
    if g // 2:
        plane = plane + 2 - 4 * (plane // 2)
    return plane


HIDE = -1e30


def attention_kernel(
    nodes,
    columns,
    neighbour_ref,
    live_ref,
    query_hbm,
    key_ref,
    value_ref,
    token_hbm,
    proj_hbm,
    router_ref,
    gain_ref,
    expert_ref,
    hidden_ref,
    normed_ref,
    gate_ref,
    level_ref,
    *scratch,
):
    chunks = D // LANES
    key_windows, value_windows = scratch[:chunks], scratch[chunks : 2 * chunks]
    own_sem, x_send, x_recv, z_send, z_recv, attn_ref = scratch[2 * chunks : 2 * chunks + 6]
    query_ref, token_ref, proj_ref, load_sem = scratch[2 * chunks + 6 : 2 * chunks + 10]
    bias_ref, weight_ref, count_ref, peers_ref, level_send, level_recv = scratch[2 * chunks + 10 :]
    devices = nodes * columns
    token_load = pltpu.make_async_copy(token_hbm, token_ref, load_sem.at[0])
    proj_load = pltpu.make_async_copy(proj_hbm, proj_ref, load_sem.at[1])
    query_load = pltpu.make_async_copy(query_hbm, query_ref, load_sem.at[2])
    node = lax.axis_index("node")
    me = node * columns + lax.axis_index("expert")
    odd = node % 2
    partner = node + 1 - 2 * odd
    onward = (node + 2 - 4 * odd + nodes) % nodes
    tiles = key_windows[0].shape[0] // 3
    barrier = pltpu.get_barrier_semaphore()

    def place(device):
        return {"node": device // columns, "expert": device % columns}

    def greet(k, carry):
        pl.semaphore_signal(
            barrier,
            inc=1,
            device_id=place((me + k) % devices),
            device_id_type=pl.DeviceIdType.MESH,
        )
        return carry

    lax.fori_loop(1, devices, greet, 0)

    members = devices // GROUPS
    plane = me // members
    wanted_plane = expert_ref[...] // members
    most = jnp.zeros((1, 1), jnp.float32)
    for g in RELAYED:
        there = jnp.where(wanted_plane == across(plane, g), 1.0, 0.0)
        most = jnp.maximum(most, jnp.sum(there, axis=1, keepdims=True))
    count_ref[...] = jnp.broadcast_to(most, count_ref.shape)
    peers_ref[me] = jnp.broadcast_to(most, count_ref.shape)

    own, first, second = [], [], []
    for c in range(chunks):
        lanes = pl.ds(c * LANES, LANES)
        for s, (source, window) in enumerate(
            ((key_ref, key_windows[c]), (value_ref, value_windows[c]))
        ):
            block = source.at[:, :, lanes]
            own.append(
                pltpu.make_async_copy(block, window.at[pl.ds(0, tiles)], own_sem.at[2 * c + s])
            )
            first.append(
                pltpu.make_async_remote_copy(
                    src_ref=block,
                    dst_ref=window.at[pl.ds(tiles, tiles)],
                    send_sem=x_send.at[2 * c + s],
                    recv_sem=x_recv.at[2 * c + s],
                    device_id={"node": partner},
                    device_id_type=pl.DeviceIdType.MESH,
                )
            )
            second.append(
                pltpu.make_async_remote_copy(
                    src_ref=window.at[pl.ds(tiles, tiles)],
                    dst_ref=window.at[pl.ds(2 * tiles, tiles)],
                    send_sem=z_send.at[2 * c + s],
                    recv_sem=z_recv.at[2 * c + s],
                    device_id={"node": onward},
                    device_id_type=pl.DeviceIdType.MESH,
                )
            )

    def tell(k, source):
        return pltpu.make_async_remote_copy(
            src_ref=count_ref,
            dst_ref=peers_ref.at[source],
            send_sem=level_send.at[k],
            recv_sem=level_recv.at[k],
            device_id=place((me + k) % devices),
            device_id_type=pl.DeviceIdType.MESH,
        )

    def each_peer(act):
        def step(k, carry):
            act(k)
            return carry

        lax.fori_loop(1, devices, step, 0)

    pl.semaphore_wait(barrier, devices - 1)
    for copy in first:
        copy.start()
    for copy in own + [token_load, query_load, proj_load]:
        copy.start()
    each_peer(lambda k: tell(k, me).start())
    for t in range(tiles):
        for j in range(NB):
            hide = jnp.where(live_ref[t, j] > 0, 0.0, HIDE)
            bias_ref[t, j * TILE : (j + 1) * TILE, :] = jnp.full(
                (TILE, LANES), hide, jnp.float32
            ).astype(jnp.bfloat16)
    token_load.wait()
    hidden_ref[...] = token_ref[...].astype(jnp.float32)
    lane = lax.broadcasted_iota(jnp.int32, (TILE, LANES), 1)
    low = lane < HEAD_DIM
    mark = (lax.broadcasted_iota(jnp.int32, (2 * TILE, LANES), 1) == 0).astype(jnp.bfloat16)
    ones = jnp.ones((NB * TILE, LANES), jnp.bfloat16)

    def position(t, j):
        listed = neighbour_ref[t, j]
        owner = listed // (tiles * columns)
        block = jnp.where(owner == node, 0, jnp.where(owner == partner, 1, 2))
        return block * tiles + listed % tiles

    def scores_of(c, t):
        query = query_ref[t * TILE : (t + 1) * TILE, c * LANES : (c + 1) * LANES]
        query = query * jnp.bfloat16(score_scale)
        blank = jnp.zeros_like(query)
        mine = jnp.concatenate(
            [jnp.where(low, query, blank), jnp.where(low, blank, query)], axis=0
        )
        near_keys = jnp.concatenate(
            [key_windows[c][position(t, j)] for j in range(NB)], axis=0
        )
        scores = lax.dot_general(
            jnp.concatenate([mine, mark], axis=1),
            jnp.concatenate([near_keys, bias_ref[t]], axis=1),
            (((1,), (1,)), ((), ())),
            preferred_element_type=jnp.float32,
        )
        peak = jnp.max(scores, axis=-1, keepdims=True)
        weight_ref[t] = jnp.exp(scores - peak).astype(jnp.bfloat16)

    def values_of(c, t):
        near_values = jnp.concatenate(
            [value_windows[c][position(t, j)] for j in range(NB)], axis=0
        )
        out = jnp.dot(
            weight_ref[t],
            jnp.concatenate([near_values, ones], axis=1),
            preferred_element_type=jnp.float32,
        )
        share = out[:, :LANES] / out[:, LANES:]
        attn_ref[t * TILE : (t + 1) * TILE, :] = jnp.where(
            low, share[:TILE], share[TILE:]
        ).astype(jnp.bfloat16)

    def relay(i):
        if i < 2 * chunks:
            first[i].wait_recv()
            second[i].start()

    query_load.wait()
    proj_load.wait()
    relay(0)
    for c in range(chunks):
        relay(2 * c + 1)
        own[2 * c].wait()
        second[2 * c].wait_recv()
        for t in range(tiles):
            if t == tiles - 1:
                relay(2 * c + 2)
            scores_of(c, t)
        own[2 * c + 1].wait()
        if c == chunks - 1:
            each_peer(lambda k: tell(k, (me - k + devices) % devices).wait_recv())
            level_ref[...] = jnp.max(peers_ref[...], axis=0)
            for copy in first:
                copy.wait_send()
            each_peer(lambda k: tell(k, me).wait_send())
        second[2 * c + 1].wait_recv()
        for t in range(tiles):
            values_of(c, t)
        hidden_ref[...] += jnp.dot(
            attn_ref[...],
            proj_ref[c * LANES : (c + 1) * LANES, :],
            preferred_element_type=jnp.float32,
        )

    def finish(t, carry):
        rows = pl.ds(pl.multiple_of(t * TILE, TILE), TILE)
        hidden = hidden_ref[rows, :]
        spread = jnp.mean(hidden * hidden, axis=-1, keepdims=True)
        normed = (hidden * lax.rsqrt(spread + 1e-06) * gain_ref[...]).astype(jnp.bfloat16)
        normed_ref[rows, :] = normed
        logits = lax.dot_general(
            normed,
            router_ref[...],
            (((1,), (1,)), ((), ())),
            preferred_element_type=jnp.float32,
        )
        experts = logits.shape[1]
        wanted = jnp.transpose(
            jnp.broadcast_to(expert_ref[:, rows].astype(jnp.float32), (TILE, TILE))
        )[:, :experts]
        column = lax.broadcasted_iota(jnp.int32, (TILE, experts), 1).astype(jnp.float32)
        chosen = jnp.sum(jnp.where(wanted == column, logits, 0.0), axis=-1, keepdims=True)
        gate_ref[rows, :] = jnp.broadcast_to(jax.nn.sigmoid(chosen), (TILE, LANES))
        return carry

    lax.fori_loop(0, tiles, finish, 0)
    for copy in second:
        copy.wait_send()


def attention_block(
    tokens, queries, keys, values, neighbours, live_bits, out_proj, norm_gain, router, expert
):
    tok_dev = tokens.shape[0]
    tiles = tok_dev // TILE
    chunks = D // LANES
    devices = lax.axis_size("node") * lax.axis_size("expert")
    window = pltpu.VMEM((3 * tiles, TILE, LANES), jnp.bfloat16)
    sems = pltpu.SemaphoreType.DMA((2 * chunks,))
    vmem = pl.BlockSpec(memory_space=pltpu.VMEM)
    smem = pl.BlockSpec(memory_space=pltpu.SMEM)
    anywhere = pl.BlockSpec(memory_space=pl.ANY)
    return pl.pallas_call(
        functools.partial(attention_kernel, lax.axis_size("node"), lax.axis_size("expert")),
        out_shape=(
            jax.ShapeDtypeStruct((tok_dev, D), jnp.float32),
            jax.ShapeDtypeStruct((tok_dev, D), jnp.bfloat16),
            jax.ShapeDtypeStruct((tok_dev, LANES), jnp.float32),
            jax.ShapeDtypeStruct((8, LANES), jnp.float32),
        ),
        in_specs=[smem, smem] + [anywhere] * 5 + [vmem] * 3,
        out_specs=(vmem,) * 4,
        scratch_shapes=[window] * (2 * chunks)
        + [sems] * 5
        + [
            pltpu.VMEM((tok_dev, LANES), jnp.bfloat16),
            pltpu.VMEM((tok_dev, D), jnp.bfloat16),
            pltpu.VMEM((tok_dev, D), jnp.bfloat16),
            pltpu.VMEM((D, D), jnp.bfloat16),
            pltpu.SemaphoreType.DMA((3,)),
            pltpu.VMEM((tiles, NB * TILE, LANES), jnp.bfloat16),
            pltpu.VMEM((tiles, 2 * TILE, NB * TILE), jnp.bfloat16),
            pltpu.VMEM((8, LANES), jnp.float32),
            pltpu.VMEM((devices, 8, LANES), jnp.float32),
            pltpu.SemaphoreType.DMA((devices,)),
            pltpu.SemaphoreType.DMA((devices,)),
        ],
        compiler_params=pltpu.CompilerParams(
            collective_id=0, has_side_effects=True, vmem_limit_bytes=62 * 1024 * 1024
        ),
    )(
        neighbours,
        live_bits,
        queries,
        keys.reshape(tiles, TILE, D),
        values.reshape(tiles, TILE, D),
        tokens,
        out_proj,
        router.T,
        norm_gain.reshape(1, D),
        expert.reshape(1, tok_dev),
    )


SPAN = 256


def expert_kernel(
    nodes, columns, outgoing_ref, up_ref, down_ref, back_ref, *scratch
):
    (
        rows_ref,
        result_ref,
        up_held,
        down_held,
        total_ref,
        weight_sem,
        own_sem,
        there_send,
        there_recv,
        back_send,
        back_recv,
    ) = scratch
    devices = nodes * columns
    cap = outgoing_ref.shape[1]
    members = devices // GROUPS
    me = lax.axis_index("node") * columns + lax.axis_index("expert")
    up_copy = pltpu.make_async_copy(up_ref.at[0], up_held, weight_sem.at[0])
    down_copy = pltpu.make_async_copy(down_ref.at[0], down_held, weight_sem.at[1])

    def place(device):
        return {"node": device // columns, "expert": device % columns}

    barrier = pltpu.get_barrier_semaphore()

    def greet(k, carry):
        pl.semaphore_signal(
            barrier,
            inc=1,
            device_id=place((me + k) % devices),
            device_id_type=pl.DeviceIdType.MESH,
        )
        return carry

    lax.fori_loop(1, devices, greet, 0)
    pl.semaphore_wait(barrier, devices - 1)

    def block(g, j):
        return pl.ds(pl.multiple_of(j * cap, cap), cap)

    def there(i):
        g, j = i // members, i % members
        target = (me + g + GROUPS * j) % devices
        return pltpu.make_async_remote_copy(
            src_ref=outgoing_ref.at[target],
            dst_ref=rows_ref.at[g, block(g, j)],
            send_sem=there_send.at[i],
            recv_sem=there_recv.at[i],
            device_id=place(target),
            device_id_type=pl.DeviceIdType.MESH,
        )

    def back(i):
        g, j = i // members, i % members
        target = (me + devices - g - GROUPS * j) % devices
        return pltpu.make_async_remote_copy(
            src_ref=result_ref.at[g, block(g, j)],
            dst_ref=back_ref.at[me],
            send_sem=back_send.at[i],
            recv_sem=back_recv.at[i],
            device_id=place(target),
            device_id_type=pl.DeviceIdType.MESH,
        )

    def back_from(i):
        g, j = i // members, i % members
        source = (me + g + GROUPS * j) % devices
        return pltpu.make_async_remote_copy(
            src_ref=result_ref.at[g, block(g, j)],
            dst_ref=back_ref.at[source],
            send_sem=back_send.at[i],
            recv_sem=back_recv.at[i],
            device_id=place(source),
            device_id_type=pl.DeviceIdType.MESH,
        )

    def each(lower, upper, act):
        def step(i, carry):
            act(i)
            return carry

        lax.fori_loop(lower, upper, step, 0)

    each(1, devices, lambda i: there(i).start())
    up_copy.start()
    down_copy.start()
    own_rows = pltpu.make_async_copy(
        outgoing_ref.at[me], rows_ref.at[0, pl.ds(0, cap)], own_sem.at[0]
    )
    own_rows.start()
    own_back = pltpu.make_async_copy(
        result_ref.at[0, pl.ds(0, cap)], back_ref.at[me], own_sem.at[1]
    )
    spans = up_held.shape[1] // SPAN
    own_rows.wait()
    up_copy.wait()
    down_copy.wait()

    def group(g, carry):
        first = jnp.maximum(g * members, 1)
        each(first, (g + 1) * members, lambda i: there(i).wait_recv())

        def span(f, inner):
            part = pl.ds(pl.multiple_of(f * SPAN, SPAN), SPAN)
            lifted = jnp.dot(rows_ref[g], up_held[:, part], preferred_element_type=jnp.float32)
            lifted = jax.nn.gelu(lifted, approximate=True).astype(jnp.bfloat16)
            total_ref[...] += jnp.dot(
                lifted, down_held[part, :], preferred_element_type=jnp.float32
            )
            return inner

        total_ref[...] = jnp.zeros_like(total_ref)
        lax.fori_loop(0, spans, span, 0)
        result_ref[g] = total_ref[...].astype(jnp.bfloat16)
        each(first, (g + 1) * members, lambda i: back(i).start())
        return carry

    lax.fori_loop(0, GROUPS, group, 0)
    own_back.start()
    own_back.wait()
    each(1, devices, lambda i: there(i).wait_send())
    each(1, devices, lambda i: back(i).wait_send())
    each(1, devices, lambda i: back_from(i).wait_recv())


def expert_exchange(outgoing, w_up, w_down):
    devices, cap, _ = outgoing.shape
    hidden_units = w_up.shape[2]
    rows = devices // GROUPS * cap
    anywhere = pl.BlockSpec(memory_space=pl.ANY)
    sems = pltpu.SemaphoreType.DMA((devices,))
    pair = pltpu.SemaphoreType.DMA((2,))
    return pl.pallas_call(
        functools.partial(expert_kernel, lax.axis_size("node"), lax.axis_size("expert")),
        out_shape=jax.ShapeDtypeStruct(outgoing.shape, jnp.bfloat16),
        in_specs=[anywhere] * 3,
        out_specs=anywhere,
        scratch_shapes=[
            pltpu.VMEM((GROUPS, rows, D), jnp.bfloat16),
            pltpu.VMEM((GROUPS, rows, D), jnp.bfloat16),
            pltpu.VMEM((D, hidden_units), jnp.bfloat16),
            pltpu.VMEM((hidden_units, D), jnp.bfloat16),
            pltpu.VMEM((rows, D), jnp.float32),
            pair,
            pair,
            sems,
            sems,
            sems,
            sems,
        ],
        compiler_params=pltpu.CompilerParams(
            collective_id=1, has_side_effects=True, vmem_limit_bytes=62 * 1024 * 1024
        ),
    )(outgoing, w_up, w_down)


WIDE = 512


def relay_kernel(
    nodes,
    columns,
    normed_ref,
    hidden_hbm,
    gate_ref,
    expert_ref,
    slot_ref,
    up_ref,
    down_ref,
    out_ref,
    up_held,
    down_held,
    hidden_ref,
    total_ref,
    lifted_ref,
    mixed_ref,
    packed_ref,
    guide_ref,
    taken_ref,
    taken_guide_ref,
    padded_ref,
    rows_ref,
    result_ref,
    back_ref,
    repacked_ref,
    home_ref,
    load_sem,
    hop_send,
    hop_recv,
    guide_send,
    guide_recv,
    home_send,
    home_recv,
    there_send,
    there_recv,
    back_send,
    back_recv,
):
    devices = nodes * columns
    members = devices // GROUPS
    tok_dev = normed_ref.shape[0]
    fit = packed_ref.shape[1]
    block = rows_ref.shape[1] // members
    cells = members * block
    me = lax.axis_index("node") * columns + lax.axis_index("expert")
    plane, member = me // members, me % members
    up_copy = pltpu.make_async_copy(up_ref.at[0], up_held, load_sem.at[0])
    down_copy = pltpu.make_async_copy(down_ref.at[0], down_held, load_sem.at[1])
    hidden_copy = pltpu.make_async_copy(hidden_hbm, hidden_ref, load_sem.at[2])

    def place(device):
        return {"node": device // columns, "expert": device % columns}

    def member_of(g, j):
        return place(across(plane, g) * members + j % members)

    def mate(g):
        return member_of(g, member)

    barrier = pltpu.get_barrier_semaphore()
    greeted = [mate(g) for g in RELAYED]
    greeted += [member_of(0, member + k) for k in range(1, members)]
    greeted += [member_of(1, member + k) for k in range(members)]
    for target in greeted:
        pl.semaphore_signal(
            barrier, inc=1, device_id=target, device_id_type=pl.DeviceIdType.MESH
        )
    up_copy.start()
    down_copy.start()
    hidden_copy.start()

    wanted = expert_ref[...] // members
    cell = expert_ref[...] % members * block + slot_ref[...]
    lines = lax.broadcasted_iota(jnp.int32, (8, tok_dev), 0)
    earlier = (
        lax.broadcasted_iota(jnp.int32, (tok_dev, tok_dev), 0)
        < lax.broadcasted_iota(jnp.int32, (tok_dev, tok_dev), 1)
    ).astype(jnp.bfloat16)
    ranks = jnp.dot(
        (
            ((lines == RELAYED[0]) & (wanted == across(plane, RELAYED[0])))
            | ((lines == RELAYED[1]) & (wanted == across(plane, RELAYED[1])))
        ).astype(jnp.bfloat16),
        earlier,
        preferred_element_type=jnp.float32,
    ).astype(jnp.int32)
    cell_lines = jnp.broadcast_to((cell + 1).astype(jnp.float32), (8, tok_dev)).astype(
        jnp.bfloat16
    )
    seats = [
        jnp.where(wanted == across(plane, g), ranks[g : g + 1, :] if g in RELAYED else cell, -1)
        for g in range(GROUPS)
    ]

    def spread(g, count):
        return (lax.broadcasted_iota(jnp.int32, (count, tok_dev), 0) == seats[g]).astype(
            jnp.bfloat16
        )

    def hop(g):
        return pltpu.make_async_remote_copy(
            src_ref=packed_ref.at[g - 2],
            dst_ref=taken_ref.at[g - 2],
            send_sem=hop_send.at[g],
            recv_sem=hop_recv.at[g],
            device_id=mate(g),
            device_id_type=pl.DeviceIdType.MESH,
        )

    def guide(g):
        return pltpu.make_async_remote_copy(
            src_ref=guide_ref.at[g - 2],
            dst_ref=taken_guide_ref.at[g - 2],
            send_sem=guide_send.at[g],
            recv_sem=guide_recv.at[g],
            device_id=mate(g),
            device_id_type=pl.DeviceIdType.MESH,
        )

    def homeward(g):
        return pltpu.make_async_remote_copy(
            src_ref=repacked_ref.at[g - 2],
            dst_ref=home_ref.at[g - 2],
            send_sem=home_send.at[g],
            recv_sem=home_recv.at[g],
            device_id=mate(g),
            device_id_type=pl.DeviceIdType.MESH,
        )

    def part(k):
        return pl.ds(pl.multiple_of(k % members * block, block), block)

    def there(g, k, source):
        return pltpu.make_async_remote_copy(
            src_ref=padded_ref.at[g, part(member + k)],
            dst_ref=rows_ref.at[g, part(source)],
            send_sem=there_send.at[g, k],
            recv_sem=there_recv.at[g, k],
            device_id=member_of(g % 2 if g < 2 else 0, member + k),
            device_id_type=pl.DeviceIdType.MESH,
        )

    def back(g, k, source):
        return pltpu.make_async_remote_copy(
            src_ref=result_ref.at[g, part(member + k)],
            dst_ref=back_ref.at[g, part(source)],
            send_sem=back_send.at[g, k],
            recv_sem=back_recv.at[g, k],
            device_id=member_of(g % 2 if g < 2 else 0, member + k),
            device_id_type=pl.DeviceIdType.MESH,
        )

    def each(g, act):
        def step(k, carry):
            act(k)
            return carry

        lax.fori_loop(0 if g == 1 else 1, members, step, 0)

    def hand_out(g):
        each(g, lambda k: there(g, k, member).start())
        if g != 1:
            rows_ref[g, part(member), :] = padded_ref[g, part(member), :]

    def placing(g):
        return (
            lax.broadcasted_iota(jnp.int32, (cells, fit), 0).astype(jnp.float32) + 1.0
            == taken_guide_ref[g - 2, 0:1, :]
        ).astype(jnp.bfloat16)

    def expand(g):
        guide(g).wait_recv()
        hop(g).wait_recv()
        padded_ref[g] = jnp.dot(
            placing(g), taken_ref[g - 2], preferred_element_type=jnp.float32
        ).astype(jnp.bfloat16)
        hand_out(g)

    def compute(g, wide):
        each(g, lambda k: there(g, k, member + members - k).wait_recv())
        spans = up_held.shape[1] // wide

        def lift(f, slot):
            part_f = pl.ds(pl.multiple_of(f * wide, wide), wide)
            lifted = jnp.dot(
                rows_ref[g], up_held[:, part_f], preferred_element_type=jnp.float32
            )
            lifted_ref[slot, :, :wide] = jax.nn.gelu(lifted, approximate=True).astype(jnp.bfloat16)

        def lower(f, slot):
            part_f = pl.ds(pl.multiple_of(f * wide, wide), wide)
            total_ref[...] += jnp.dot(
                lifted_ref[slot, :, :wide], down_held[part_f, :], preferred_element_type=jnp.float32
            )

        def span(i, carry):
            lift(2 * i + 1, 1)
            lower(2 * i, 0)
            lift(2 * i + 2, 0)
            lower(2 * i + 1, 1)
            return carry

        total_ref[...] = jnp.zeros_like(total_ref)
        lift(0, 0)
        lax.fori_loop(0, spans // 2 - 1, span, 0)
        lift(spans - 1, 1)
        lower(spans - 2, 0)
        lower(spans - 1, 1)
        result_ref[g] = total_ref[...].astype(jnp.bfloat16)

    def reply(g):
        each(g, lambda k: back(g, k, member).start())
        if g != 1:
            back_ref[g, part(member), :] = result_ref[g, part(member), :]

    def collect(g):
        each(g, lambda k: back(g, k, member + members - k).wait_recv())

    def repack(g):
        collect(g)
        repacked_ref[g - 2] = lax.dot_general(
            placing(g),
            back_ref[g],
            (((0,), (0,)), ((), ())),
            preferred_element_type=jnp.float32,
        ).astype(jnp.bfloat16)
        homeward(g).start()

    def take_home(g, source, count):
        seated = spread(g, count)
        return lax.dot_general(
            seated, source, (((0,), (0,)), ((), ())), preferred_element_type=jnp.float32
        )

    def pack(g):
        seated = spread(g, fit)
        packed_ref[g - 2] = jnp.dot(
            seated, normed_ref[...], preferred_element_type=jnp.float32
        ).astype(jnp.bfloat16)
        guide_ref[g - 2] = lax.dot_general(
            cell_lines, seated, (((1,), (1,)), ((), ())), preferred_element_type=jnp.float32
        )

    def pad(g):
        padded_ref[g] = jnp.dot(
            spread(g, cells), normed_ref[...], preferred_element_type=jnp.float32
        ).astype(jnp.bfloat16)

    near, far = RELAYED
    pad(1)
    pl.semaphore_wait(barrier, len(greeted))
    hand_out(1)
    pad(0)
    hand_out(0)
    pack(near)
    guide(near).start()
    hop(near).start()
    pack(far)
    up_copy.wait()
    down_copy.wait()
    compute(0, WIDE // 2)
    reply(0)
    hop(near).wait_send()
    guide(far).start()
    hop(far).start()
    expand(near)
    compute(1, WIDE // 2)
    reply(1)
    compute(near, WIDE)
    reply(near)
    collect(0)
    mixed_ref[...] = take_home(0, back_ref[0], cells)
    expand(far)
    collect(1)
    mixed_ref[...] += take_home(1, back_ref[1], cells)
    repack(near)
    compute(far, WIDE)
    reply(far)
    repack(far)
    hidden_copy.wait()
    homeward(near).wait_recv()
    mixed_ref[...] += take_home(near, home_ref[near - 2], fit)
    homeward(far).wait_recv()
    mixed = mixed_ref[...] + take_home(far, home_ref[far - 2], fit)
    out_ref[...] = (hidden_ref[...] + gate_ref[:, 0:1] * mixed).astype(jnp.bfloat16)
    for g in range(GROUPS):
        each(g, lambda k: there(g, k, member).wait_send())
        each(g, lambda k: back(g, k, member).wait_send())
    hop(far).wait_send()
    for g in RELAYED:
        guide(g).wait_send()
        homeward(g).wait_send()


def relay_exchange(fit, normed, hidden, gate, expert, slot, w_up, w_down):
    tok_dev = normed.shape[0]
    hidden_units = w_up.shape[2]
    nodes, columns = lax.axis_size("node"), lax.axis_size("expert")
    members = nodes * columns // GROUPS
    cells = 2 * tok_dev // GROUPS
    anywhere = pl.BlockSpec(memory_space=pl.ANY)
    vmem = pl.BlockSpec(memory_space=pltpu.VMEM)
    packed = pltpu.VMEM((len(RELAYED), fit, D), jnp.bfloat16)
    guides = pltpu.VMEM((len(RELAYED), 8, fit), jnp.float32)
    grouped = pltpu.VMEM((GROUPS, cells, D), jnp.bfloat16)
    hop_sems = pltpu.SemaphoreType.DMA((GROUPS,))
    peer_sems = pltpu.SemaphoreType.DMA((GROUPS, members))
    return pl.pallas_call(
        functools.partial(relay_kernel, nodes, columns),
        out_shape=jax.ShapeDtypeStruct((tok_dev, D), jnp.bfloat16),
        in_specs=[vmem, anywhere, vmem, vmem, vmem, anywhere, anywhere],
        out_specs=vmem,
        scratch_shapes=[
            pltpu.VMEM((D, hidden_units), jnp.bfloat16),
            pltpu.VMEM((hidden_units, D), jnp.bfloat16),
            pltpu.VMEM((tok_dev, D), jnp.float32),
            pltpu.VMEM((cells, D), jnp.float32),
            pltpu.VMEM((2, cells, WIDE), jnp.bfloat16),
            pltpu.VMEM((tok_dev, D), jnp.float32),
            packed,
            guides,
            packed,
            guides,
            grouped,
            grouped,
            grouped,
            grouped,
            packed,
            packed,
            pltpu.SemaphoreType.DMA((3,)),
        ]
        + [hop_sems] * 6
        + [peer_sems] * 4,
        compiler_params=pltpu.CompilerParams(
            collective_id=2, has_side_effects=True, vmem_limit_bytes=62 * 1024 * 1024
        ),
    )(
        normed,
        hidden,
        gate,
        expert.reshape(1, tok_dev),
        slot.reshape(1, tok_dev),
        w_up,
        w_down,
    )


def exchange_by_blocks(outgoing, w_up, w_down):
    experts, cap, _ = outgoing.shape
    block = lax.all_to_all(
        outgoing.reshape(experts, 1, cap, D),
        ("node", "expert"),
        split_axis=0,
        concat_axis=1,
        tiled=True,
    )
    token_rows = block.reshape(-1, D)
    lifted = jnp.dot(token_rows, w_up[0], preferred_element_type=jnp.float32)
    lifted = jax.nn.gelu(lifted, approximate=True).astype(jnp.bfloat16)
    result = jnp.dot(lifted, w_down[0], preferred_element_type=jnp.float32).astype(jnp.bfloat16)
    return lax.all_to_all(
        result.reshape(block.shape), ("node", "expert"), split_axis=1, concat_axis=0, tiled=True
    )


def shards(
    tokens,
    queries,
    keys,
    values,
    neighbours,
    live_bits,
    out_proj,
    norm_gain,
    router,
    expert,
    slot,
    w_up,
    w_down,
):
    tok_dev = tokens.shape[0]
    experts = router.shape[1]
    cap = 2 * tok_dev // experts
    hidden, normed, gate, level = attention_block(
        tokens, queries, keys, values, neighbours, live_bits, out_proj, norm_gain, router, expert
    )

    def padded_way():
        slot_cell = expert * cap + slot
        one_hot = (lax.iota(jnp.int32, experts * cap)[:, None] == slot_cell[None, :]).astype(
            jnp.bfloat16
        )
        outgoing = jnp.dot(one_hot, normed, preferred_element_type=jnp.float32).astype(
            jnp.bfloat16
        )
        exchange = exchange_by_blocks if cap % 16 else expert_exchange
        returned = exchange(outgoing.reshape(experts, cap, D), w_up, w_down)
        flat_back = returned.reshape(experts * cap, D)
        expert_out = jnp.einsum(
            "ct,cd->td", one_hot, flat_back, preferred_element_type=jnp.float32
        )
        layer_out = hidden + gate[:, :1] * expert_out
        return layer_out.astype(jnp.bfloat16)

    def relayed_way():
        return relay_exchange(fit, normed, hidden, gate, expert, slot, w_up, w_down)

    fit = 2 * tok_dev // GROUPS * 3 // 4
    if cap % 16 or lax.axis_size("node") % GROUPS:
        return padded_way()
    return lax.cond(level[0, 0] <= fit, relayed_way, padded_way)


def solution(mesh):
    in_specs = (
        P(("node", "expert"), None),
        P(("node", "expert"), None),
        P(("node", "expert"), None),
        P(("node", "expert"), None),
        P(("node", "expert"), None),
        P(("node", "expert"), None),
        P(),
        P(),
        P(),
        P(("node", "expert")),
        P(("node", "expert")),
        P(("node", "expert"), None, None),
        P(("node", "expert"), None, None),
    )
    out_specs = P(("node", "expert"), None)
    return jax.shard_map(shards, mesh=mesh, in_specs=in_specs, out_specs=out_specs, check_vma=False)
```

```python
import functools

import jax
import jax.numpy as jnp
from jax import lax
from jax.experimental import pallas as pl
from jax.experimental.pallas import tpu as pltpu
from jax.sharding import PartitionSpec as P

D = 1024
HEADS = 16
HEAD_DIM = 64
TILE = 128
NB = 8


score_scale = 0.125


LANES = 128
GROUPS = 4
RELAYED = (2, 3)


def across(plane, g):
    if g % 2:
        plane = plane + 1 - 2 * (plane % 2)
    if g // 2:
        plane = plane + 2 - 4 * (plane // 2)
    return plane


HIDE = -1e30


def attention_kernel(
    nodes,
    columns,
    neighbour_ref,
    live_ref,
    query_hbm,
    key_ref,
    value_ref,
    token_hbm,
    proj_hbm,
    router_ref,
    gain_ref,
    expert_ref,
    hidden_ref,
    normed_ref,
    gate_ref,
    level_ref,
    *scratch,
):
    chunks = D // LANES
    key_windows, value_windows = scratch[:chunks], scratch[chunks : 2 * chunks]
    own_sem, x_send, x_recv, z_send, z_recv, attn_ref = scratch[2 * chunks : 2 * chunks + 6]
    query_ref, token_ref, proj_ref, load_sem = scratch[2 * chunks + 6 : 2 * chunks + 10]
    bias_ref, weight_ref, count_ref, peers_ref, level_send, level_recv = scratch[2 * chunks + 10 :]
    devices = nodes * columns
    token_load = pltpu.make_async_copy(token_hbm, token_ref, load_sem.at[0])
    proj_load = pltpu.make_async_copy(proj_hbm, proj_ref, load_sem.at[1])
    query_load = pltpu.make_async_copy(query_hbm, query_ref, load_sem.at[2])
    node = lax.axis_index("node")
    me = node * columns + lax.axis_index("expert")
    odd = node % 2
    partner = node + 1 - 2 * odd
    onward = (node + 2 - 4 * odd + nodes) % nodes
    tiles = key_windows[0].shape[0] // 3
    barrier = pltpu.get_barrier_semaphore()

    def place(device):
        return {"node": device // columns, "expert": device % columns}

    def greet(k, carry):
        pl.semaphore_signal(
            barrier,
            inc=1,
            device_id=place((me + k) % devices),
            device_id_type=pl.DeviceIdType.MESH,
        )
        return carry

    lax.fori_loop(1, devices, greet, 0)

    members = devices // GROUPS
    plane = me // members
    wanted_plane = expert_ref[...] // members
    most = jnp.zeros((1, 1), jnp.float32)
    for g in RELAYED:
        there = jnp.where(wanted_plane == across(plane, g), 1.0, 0.0)
        most = jnp.maximum(most, jnp.sum(there, axis=1, keepdims=True))
    count_ref[...] = jnp.broadcast_to(most, count_ref.shape)
    peers_ref[me] = jnp.broadcast_to(most, count_ref.shape)

    own, first, second = [], [], []
    for c in range(chunks):
        lanes = pl.ds(c * LANES, LANES)
        for s, (source, window) in enumerate(
            ((key_ref, key_windows[c]), (value_ref, value_windows[c]))
        ):
            block = source.at[:, :, lanes]
            own.append(
                pltpu.make_async_copy(block, window.at[pl.ds(0, tiles)], own_sem.at[2 * c + s])
            )
            first.append(
                pltpu.make_async_remote_copy(
                    src_ref=block,
                    dst_ref=window.at[pl.ds(tiles, tiles)],
                    send_sem=x_send.at[2 * c + s],
                    recv_sem=x_recv.at[2 * c + s],
                    device_id={"node": partner},
                    device_id_type=pl.DeviceIdType.MESH,
                )
            )
            second.append(
                pltpu.make_async_remote_copy(
                    src_ref=window.at[pl.ds(tiles, tiles)],
                    dst_ref=window.at[pl.ds(2 * tiles, tiles)],
                    send_sem=z_send.at[2 * c + s],
                    recv_sem=z_recv.at[2 * c + s],
                    device_id={"node": onward},
                    device_id_type=pl.DeviceIdType.MESH,
                )
            )

    def tell(k, source):
        return pltpu.make_async_remote_copy(
            src_ref=count_ref,
            dst_ref=peers_ref.at[source],
            send_sem=level_send.at[k],
            recv_sem=level_recv.at[k],
            device_id=place((me + k) % devices),
            device_id_type=pl.DeviceIdType.MESH,
        )

    def each_peer(act):
        def step(k, carry):
            act(k)
            return carry

        lax.fori_loop(1, devices, step, 0)

    pl.semaphore_wait(barrier, devices - 1)
    for copy in first:
        copy.start()
    for copy in own + [token_load, query_load, proj_load]:
        copy.start()
    each_peer(lambda k: tell(k, me).start())
    for t in range(tiles):
        for j in range(NB):
            hide = jnp.where(live_ref[t, j] > 0, 0.0, HIDE)
            bias_ref[t, j * TILE : (j + 1) * TILE, :] = jnp.full(
                (TILE, LANES), hide, jnp.float32
            ).astype(jnp.bfloat16)
    token_load.wait()
    hidden_ref[...] = token_ref[...].astype(jnp.float32)
    lane = lax.broadcasted_iota(jnp.int32, (TILE, LANES), 1)
    low = lane < HEAD_DIM
    mark = (lax.broadcasted_iota(jnp.int32, (2 * TILE, LANES), 1) == 0).astype(jnp.bfloat16)
    ones = jnp.ones((NB * TILE, LANES), jnp.bfloat16)

    def position(t, j):
        listed = neighbour_ref[t, j]
        owner = listed // (tiles * columns)
        block = jnp.where(owner == node, 0, jnp.where(owner == partner, 1, 2))
        return block * tiles + listed % tiles

    def scores_of(c, t):
        query = query_ref[t * TILE : (t + 1) * TILE, c * LANES : (c + 1) * LANES]
        query = query * jnp.bfloat16(score_scale)
        blank = jnp.zeros_like(query)
        mine = jnp.concatenate(
            [jnp.where(low, query, blank), jnp.where(low, blank, query)], axis=0
        )
        near_keys = jnp.concatenate(
            [key_windows[c][position(t, j)] for j in range(NB)], axis=0
        )
        scores = lax.dot_general(
            jnp.concatenate([mine, mark], axis=1),
            jnp.concatenate([near_keys, bias_ref[t]], axis=1),
            (((1,), (1,)), ((), ())),
            preferred_element_type=jnp.float32,
        )
        peak = jnp.max(scores, axis=-1, keepdims=True)
        weight_ref[t] = jnp.exp(scores - peak).astype(jnp.bfloat16)

    def values_of(c, t):
        near_values = jnp.concatenate(
            [value_windows[c][position(t, j)] for j in range(NB)], axis=0
        )
        out = jnp.dot(
            weight_ref[t],
            jnp.concatenate([near_values, ones], axis=1),
            preferred_element_type=jnp.float32,
        )
        share = out[:, :LANES] / out[:, LANES:]
        attn_ref[t * TILE : (t + 1) * TILE, :] = jnp.where(
            low, share[:TILE], share[TILE:]
        ).astype(jnp.bfloat16)

    def relay(i):
        if i < 2 * chunks:
            first[i].wait_recv()
            second[i].start()

    query_load.wait()
    proj_load.wait()
    relay(0)
    for c in range(chunks):
        relay(2 * c + 1)
        own[2 * c].wait()
        second[2 * c].wait_recv()
        for t in range(tiles):
            if t == tiles - 1:
                relay(2 * c + 2)
            scores_of(c, t)
        own[2 * c + 1].wait()
        if c == chunks - 1:
            each_peer(lambda k: tell(k, (me - k + devices) % devices).wait_recv())
            level_ref[...] = jnp.max(peers_ref[...], axis=0)
            for copy in first:
                copy.wait_send()
            each_peer(lambda k: tell(k, me).wait_send())
        second[2 * c + 1].wait_recv()
        for t in range(tiles):
            values_of(c, t)
        hidden_ref[...] += jnp.dot(
            attn_ref[...],
            proj_ref[c * LANES : (c + 1) * LANES, :],
            preferred_element_type=jnp.float32,
        )

    def finish(t):
        rows = pl.ds(t * TILE, TILE)
        hidden = hidden_ref[rows, :]
        spread = jnp.mean(hidden * hidden, axis=-1, keepdims=True)
        normed = (hidden * lax.rsqrt(spread + 1e-06) * gain_ref[...]).astype(jnp.bfloat16)
        normed_ref[rows, :] = normed
        logits = lax.dot_general(
            normed,
            router_ref[...],
            (((1,), (1,)), ((), ())),
            preferred_element_type=jnp.float32,
        )
        experts = logits.shape[1]
        wanted = jnp.transpose(
            jnp.broadcast_to(expert_ref[:, rows].astype(jnp.float32), (TILE, TILE))
        )[:, :experts]
        column = lax.broadcasted_iota(jnp.int32, (TILE, experts), 1).astype(jnp.float32)
        chosen = jnp.sum(jnp.where(wanted == column, logits, 0.0), axis=-1, keepdims=True)
        gate_ref[rows, :] = jnp.broadcast_to(jax.nn.sigmoid(chosen), (TILE, LANES))

    for copy in second:
        copy.wait_send()
    for t in range(tiles):
        finish(t)


def attention_block(
    tokens, queries, keys, values, neighbours, live_bits, out_proj, norm_gain, router, expert
):
    tok_dev = tokens.shape[0]
    tiles = tok_dev // TILE
    chunks = D // LANES
    devices = lax.axis_size("node") * lax.axis_size("expert")
    window = pltpu.VMEM((3 * tiles, TILE, LANES), jnp.bfloat16)
    sems = pltpu.SemaphoreType.DMA((2 * chunks,))
    vmem = pl.BlockSpec(memory_space=pltpu.VMEM)
    smem = pl.BlockSpec(memory_space=pltpu.SMEM)
    anywhere = pl.BlockSpec(memory_space=pl.ANY)
    return pl.pallas_call(
        functools.partial(attention_kernel, lax.axis_size("node"), lax.axis_size("expert")),
        out_shape=(
            jax.ShapeDtypeStruct((tok_dev, D), jnp.float32),
            jax.ShapeDtypeStruct((tok_dev, D), jnp.bfloat16),
            jax.ShapeDtypeStruct((tok_dev, LANES), jnp.float32),
            jax.ShapeDtypeStruct((8, LANES), jnp.float32),
        ),
        in_specs=[smem, smem] + [anywhere] * 5 + [vmem] * 3,
        out_specs=(vmem,) * 4,
        scratch_shapes=[window] * (2 * chunks)
        + [sems] * 5
        + [
            pltpu.VMEM((tok_dev, LANES), jnp.bfloat16),
            pltpu.VMEM((tok_dev, D), jnp.bfloat16),
            pltpu.VMEM((tok_dev, D), jnp.bfloat16),
            pltpu.VMEM((D, D), jnp.bfloat16),
            pltpu.SemaphoreType.DMA((3,)),
            pltpu.VMEM((tiles, NB * TILE, LANES), jnp.bfloat16),
            pltpu.VMEM((tiles, 2 * TILE, NB * TILE), jnp.bfloat16),
            pltpu.VMEM((8, LANES), jnp.float32),
            pltpu.VMEM((devices, 8, LANES), jnp.float32),
            pltpu.SemaphoreType.DMA((devices,)),
            pltpu.SemaphoreType.DMA((devices,)),
        ],
        compiler_params=pltpu.CompilerParams(
            collective_id=0, has_side_effects=True, vmem_limit_bytes=62 * 1024 * 1024
        ),
    )(
        neighbours,
        live_bits,
        queries,
        keys.reshape(tiles, TILE, D),
        values.reshape(tiles, TILE, D),
        tokens,
        out_proj,
        router.T,
        norm_gain.reshape(1, D),
        expert.reshape(1, tok_dev),
    )


SPAN = 256


def expert_kernel(
    nodes, columns, outgoing_ref, up_ref, down_ref, back_ref, *scratch
):
    (
        rows_ref,
        result_ref,
        up_held,
        down_held,
        total_ref,
        weight_sem,
        own_sem,
        there_send,
        there_recv,
        back_send,
        back_recv,
    ) = scratch
    devices = nodes * columns
    cap = outgoing_ref.shape[1]
    members = devices // GROUPS
    me = lax.axis_index("node") * columns + lax.axis_index("expert")
    up_copy = pltpu.make_async_copy(up_ref.at[0], up_held, weight_sem.at[0])
    down_copy = pltpu.make_async_copy(down_ref.at[0], down_held, weight_sem.at[1])

    def place(device):
        return {"node": device // columns, "expert": device % columns}

    barrier = pltpu.get_barrier_semaphore()

    def greet(k, carry):
        pl.semaphore_signal(
            barrier,
            inc=1,
            device_id=place((me + k) % devices),
            device_id_type=pl.DeviceIdType.MESH,
        )
        return carry

    lax.fori_loop(1, devices, greet, 0)
    pl.semaphore_wait(barrier, devices - 1)

    def block(g, j):
        return pl.ds(pl.multiple_of(j * cap, cap), cap)

    def there(i):
        g, j = i // members, i % members
        target = (me + g + GROUPS * j) % devices
        return pltpu.make_async_remote_copy(
            src_ref=outgoing_ref.at[target],
            dst_ref=rows_ref.at[g, block(g, j)],
            send_sem=there_send.at[i],
            recv_sem=there_recv.at[i],
            device_id=place(target),
            device_id_type=pl.DeviceIdType.MESH,
        )

    def back(i):
        g, j = i // members, i % members
        target = (me + devices - g - GROUPS * j) % devices
        return pltpu.make_async_remote_copy(
            src_ref=result_ref.at[g, block(g, j)],
            dst_ref=back_ref.at[me],
            send_sem=back_send.at[i],
            recv_sem=back_recv.at[i],
            device_id=place(target),
            device_id_type=pl.DeviceIdType.MESH,
        )

    def back_from(i):
        g, j = i // members, i % members
        source = (me + g + GROUPS * j) % devices
        return pltpu.make_async_remote_copy(
            src_ref=result_ref.at[g, block(g, j)],
            dst_ref=back_ref.at[source],
            send_sem=back_send.at[i],
            recv_sem=back_recv.at[i],
            device_id=place(source),
            device_id_type=pl.DeviceIdType.MESH,
        )

    def each(lower, upper, act):
        def step(i, carry):
            act(i)
            return carry

        lax.fori_loop(lower, upper, step, 0)

    each(1, devices, lambda i: there(i).start())
    up_copy.start()
    down_copy.start()
    own_rows = pltpu.make_async_copy(
        outgoing_ref.at[me], rows_ref.at[0, pl.ds(0, cap)], own_sem.at[0]
    )
    own_rows.start()
    own_back = pltpu.make_async_copy(
        result_ref.at[0, pl.ds(0, cap)], back_ref.at[me], own_sem.at[1]
    )
    spans = up_held.shape[1] // SPAN
    own_rows.wait()
    up_copy.wait()
    down_copy.wait()

    def group(g, carry):
        first = jnp.maximum(g * members, 1)
        each(first, (g + 1) * members, lambda i: there(i).wait_recv())

        def span(f, inner):
            part = pl.ds(pl.multiple_of(f * SPAN, SPAN), SPAN)
            lifted = jnp.dot(rows_ref[g], up_held[:, part], preferred_element_type=jnp.float32)
            lifted = jax.nn.gelu(lifted, approximate=True).astype(jnp.bfloat16)
            total_ref[...] += jnp.dot(
                lifted, down_held[part, :], preferred_element_type=jnp.float32
            )
            return inner

        total_ref[...] = jnp.zeros_like(total_ref)
        lax.fori_loop(0, spans, span, 0)
        result_ref[g] = total_ref[...].astype(jnp.bfloat16)
        each(first, (g + 1) * members, lambda i: back(i).start())
        return carry

    lax.fori_loop(0, GROUPS, group, 0)
    own_back.start()
    own_back.wait()
    each(1, devices, lambda i: there(i).wait_send())
    each(1, devices, lambda i: back(i).wait_send())
    each(1, devices, lambda i: back_from(i).wait_recv())


def expert_exchange(outgoing, w_up, w_down):
    devices, cap, _ = outgoing.shape
    hidden_units = w_up.shape[2]
    rows = devices // GROUPS * cap
    anywhere = pl.BlockSpec(memory_space=pl.ANY)
    sems = pltpu.SemaphoreType.DMA((devices,))
    pair = pltpu.SemaphoreType.DMA((2,))
    return pl.pallas_call(
        functools.partial(expert_kernel, lax.axis_size("node"), lax.axis_size("expert")),
        out_shape=jax.ShapeDtypeStruct(outgoing.shape, jnp.bfloat16),
        in_specs=[anywhere] * 3,
        out_specs=anywhere,
        scratch_shapes=[
            pltpu.VMEM((GROUPS, rows, D), jnp.bfloat16),
            pltpu.VMEM((GROUPS, rows, D), jnp.bfloat16),
            pltpu.VMEM((D, hidden_units), jnp.bfloat16),
            pltpu.VMEM((hidden_units, D), jnp.bfloat16),
            pltpu.VMEM((rows, D), jnp.float32),
            pair,
            pair,
            sems,
            sems,
            sems,
            sems,
        ],
        compiler_params=pltpu.CompilerParams(
            collective_id=1, has_side_effects=True, vmem_limit_bytes=62 * 1024 * 1024
        ),
    )(outgoing, w_up, w_down)


WIDE = 512


def relay_kernel(
    nodes,
    columns,
    normed_ref,
    hidden_hbm,
    gate_ref,
    expert_ref,
    slot_ref,
    up_ref,
    down_ref,
    out_ref,
    up_held,
    down_held,
    hidden_ref,
    total_ref,
    lifted_ref,
    mixed_ref,
    packed_ref,
    guide_ref,
    taken_ref,
    taken_guide_ref,
    padded_ref,
    rows_ref,
    result_ref,
    back_ref,
    repacked_ref,
    home_ref,
    load_sem,
    hop_send,
    hop_recv,
    guide_send,
    guide_recv,
    home_send,
    home_recv,
    there_send,
    there_recv,
    back_send,
    back_recv,
):
    devices = nodes * columns
    members = devices // GROUPS
    tok_dev = normed_ref.shape[0]
    fit = packed_ref.shape[1]
    block = rows_ref.shape[1] // members
    cells = members * block
    me = lax.axis_index("node") * columns + lax.axis_index("expert")
    plane, member = me // members, me % members
    up_copy = pltpu.make_async_copy(up_ref.at[0], up_held, load_sem.at[0])
    down_copy = pltpu.make_async_copy(down_ref.at[0], down_held, load_sem.at[1])
    hidden_copy = pltpu.make_async_copy(hidden_hbm, hidden_ref, load_sem.at[2])

    def place(device):
        return {"node": device // columns, "expert": device % columns}

    def member_of(g, j):
        return place(across(plane, g) * members + j % members)

    def mate(g):
        return member_of(g, member)

    barrier = pltpu.get_barrier_semaphore()
    greeted = [mate(g) for g in RELAYED]
    greeted += [member_of(0, member + k) for k in range(1, members)]
    greeted += [member_of(1, member + k) for k in range(members)]
    for target in greeted:
        pl.semaphore_signal(
            barrier, inc=1, device_id=target, device_id_type=pl.DeviceIdType.MESH
        )
    up_copy.start()
    down_copy.start()
    hidden_copy.start()

    wanted = expert_ref[...] // members
    cell = expert_ref[...] % members * block + slot_ref[...]
    lines = lax.broadcasted_iota(jnp.int32, (8, tok_dev), 0)
    earlier = (
        lax.broadcasted_iota(jnp.int32, (tok_dev, tok_dev), 0)
        < lax.broadcasted_iota(jnp.int32, (tok_dev, tok_dev), 1)
    ).astype(jnp.bfloat16)
    ranks = jnp.dot(
        (
            ((lines == RELAYED[0]) & (wanted == across(plane, RELAYED[0])))
            | ((lines == RELAYED[1]) & (wanted == across(plane, RELAYED[1])))
        ).astype(jnp.bfloat16),
        earlier,
        preferred_element_type=jnp.float32,
    ).astype(jnp.int32)
    cell_lines = jnp.broadcast_to((cell + 1).astype(jnp.float32), (8, tok_dev)).astype(
        jnp.bfloat16
    )
    seats = [
        jnp.where(wanted == across(plane, g), ranks[g : g + 1, :] if g in RELAYED else cell, -1)
        for g in range(GROUPS)
    ]

    def spread(g, count):
        return (lax.broadcasted_iota(jnp.int32, (count, tok_dev), 0) == seats[g]).astype(
            jnp.bfloat16
        )

    def hop(g):
        return pltpu.make_async_remote_copy(
            src_ref=packed_ref.at[g - 2],
            dst_ref=taken_ref.at[g - 2],
            send_sem=hop_send.at[g],
            recv_sem=hop_recv.at[g],
            device_id=mate(g),
            device_id_type=pl.DeviceIdType.MESH,
        )

    def guide(g):
        return pltpu.make_async_remote_copy(
            src_ref=guide_ref.at[g - 2],
            dst_ref=taken_guide_ref.at[g - 2],
            send_sem=guide_send.at[g],
            recv_sem=guide_recv.at[g],
            device_id=mate(g),
            device_id_type=pl.DeviceIdType.MESH,
        )

    def homeward(g):
        return pltpu.make_async_remote_copy(
            src_ref=repacked_ref.at[g - 2],
            dst_ref=home_ref.at[g - 2],
            send_sem=home_send.at[g],
            recv_sem=home_recv.at[g],
            device_id=mate(g),
            device_id_type=pl.DeviceIdType.MESH,
        )

    def part(k):
        return pl.ds(pl.multiple_of(k % members * block, block), block)

    def there(g, k, source):
        return pltpu.make_async_remote_copy(
            src_ref=padded_ref.at[g, part(member + k)],
            dst_ref=rows_ref.at[g, part(source)],
            send_sem=there_send.at[g, k],
            recv_sem=there_recv.at[g, k],
            device_id=member_of(g % 2 if g < 2 else 0, member + k),
            device_id_type=pl.DeviceIdType.MESH,
        )

    def back(g, k, source):
        return pltpu.make_async_remote_copy(
            src_ref=result_ref.at[g, part(member + k)],
            dst_ref=back_ref.at[g, part(source)],
            send_sem=back_send.at[g, k],
            recv_sem=back_recv.at[g, k],
            device_id=member_of(g % 2 if g < 2 else 0, member + k),
            device_id_type=pl.DeviceIdType.MESH,
        )

    def each(g, act):
        def step(k, carry):
            act(k)
            return carry

        lax.fori_loop(0 if g == 1 else 1, members, step, 0)

    def hand_out(g):
        each(g, lambda k: there(g, k, member).start())
        if g != 1:
            rows_ref[g, part(member), :] = padded_ref[g, part(member), :]

    def placing(g):
        return (
            lax.broadcasted_iota(jnp.int32, (cells, fit), 0).astype(jnp.float32) + 1.0
            == taken_guide_ref[g - 2, 0:1, :]
        ).astype(jnp.bfloat16)

    def expand(g):
        guide(g).wait_recv()
        hop(g).wait_recv()
        padded_ref[g] = jnp.dot(
            placing(g), taken_ref[g - 2], preferred_element_type=jnp.float32
        ).astype(jnp.bfloat16)
        hand_out(g)

    def compute(g, wide):
        each(g, lambda k: there(g, k, member + members - k).wait_recv())
        spans = up_held.shape[1] // wide

        def lift(f, slot):
            part_f = pl.ds(pl.multiple_of(f * wide, wide), wide)
            lifted = jnp.dot(
                rows_ref[g], up_held[:, part_f], preferred_element_type=jnp.float32
            )
            lifted_ref[slot, :, :wide] = jax.nn.gelu(lifted, approximate=True).astype(jnp.bfloat16)

        def lower(f, slot):
            part_f = pl.ds(pl.multiple_of(f * wide, wide), wide)
            total_ref[...] += jnp.dot(
                lifted_ref[slot, :, :wide], down_held[part_f, :], preferred_element_type=jnp.float32
            )

        def span(i, carry):
            lift(2 * i + 1, 1)
            lower(2 * i, 0)
            lift(2 * i + 2, 0)
            lower(2 * i + 1, 1)
            return carry

        total_ref[...] = jnp.zeros_like(total_ref)
        lift(0, 0)
        lax.fori_loop(0, spans // 2 - 1, span, 0)
        lift(spans - 1, 1)
        lower(spans - 2, 0)
        lower(spans - 1, 1)
        result_ref[g] = total_ref[...].astype(jnp.bfloat16)

    def reply(g):
        each(g, lambda k: back(g, k, member).start())
        if g != 1:
            back_ref[g, part(member), :] = result_ref[g, part(member), :]

    def collect(g):
        each(g, lambda k: back(g, k, member + members - k).wait_recv())

    def repack(g):
        collect(g)
        repacked_ref[g - 2] = lax.dot_general(
            placing(g),
            back_ref[g],
            (((0,), (0,)), ((), ())),
            preferred_element_type=jnp.float32,
        ).astype(jnp.bfloat16)
        homeward(g).start()

    def take_home(g, source, count):
        seated = spread(g, count)
        return lax.dot_general(
            seated, source, (((0,), (0,)), ((), ())), preferred_element_type=jnp.float32
        )

    def pack(g):
        seated = spread(g, fit)
        packed_ref[g - 2] = jnp.dot(
            seated, normed_ref[...], preferred_element_type=jnp.float32
        ).astype(jnp.bfloat16)
        guide_ref[g - 2] = lax.dot_general(
            cell_lines, seated, (((1,), (1,)), ((), ())), preferred_element_type=jnp.float32
        )

    def pad(g):
        padded_ref[g] = jnp.dot(
            spread(g, cells), normed_ref[...], preferred_element_type=jnp.float32
        ).astype(jnp.bfloat16)

    near, far = RELAYED
    pad(1)
    pl.semaphore_wait(barrier, len(greeted))
    hand_out(1)
    pad(0)
    hand_out(0)
    pack(near)
    guide(near).start()
    hop(near).start()
    pack(far)
    up_copy.wait()
    down_copy.wait()
    compute(0, WIDE // 2)
    reply(0)
    hop(near).wait_send()
    guide(far).start()
    hop(far).start()
    expand(near)
    compute(1, WIDE // 2)
    reply(1)
    compute(near, WIDE)
    reply(near)
    collect(0)
    mixed_ref[...] = take_home(0, back_ref[0], cells)
    expand(far)
    collect(1)
    mixed_ref[...] += take_home(1, back_ref[1], cells)
    repack(near)
    compute(far, WIDE)
    reply(far)
    repack(far)
    for g in range(GROUPS):
        each(g, lambda k: there(g, k, member).wait_send())
        each(g, lambda k: back(g, k, member).wait_send())
    hidden_copy.wait()
    homeward(near).wait_recv()
    mixed_ref[...] += take_home(near, home_ref[near - 2], fit)
    homeward(far).wait_recv()
    mixed = mixed_ref[...] + take_home(far, home_ref[far - 2], fit)
    out_ref[...] = (hidden_ref[...] + gate_ref[:, 0:1] * mixed).astype(jnp.bfloat16)
    hop(far).wait_send()
    for g in RELAYED:
        guide(g).wait_send()
        homeward(g).wait_send()


def relay_exchange(fit, normed, hidden, gate, expert, slot, w_up, w_down):
    tok_dev = normed.shape[0]
    hidden_units = w_up.shape[2]
    nodes, columns = lax.axis_size("node"), lax.axis_size("expert")
    members = nodes * columns // GROUPS
    cells = 2 * tok_dev // GROUPS
    anywhere = pl.BlockSpec(memory_space=pl.ANY)
    vmem = pl.BlockSpec(memory_space=pltpu.VMEM)
    packed = pltpu.VMEM((len(RELAYED), fit, D), jnp.bfloat16)
    guides = pltpu.VMEM((len(RELAYED), 8, fit), jnp.float32)
    grouped = pltpu.VMEM((GROUPS, cells, D), jnp.bfloat16)
    hop_sems = pltpu.SemaphoreType.DMA((GROUPS,))
    peer_sems = pltpu.SemaphoreType.DMA((GROUPS, members))
    return pl.pallas_call(
        functools.partial(relay_kernel, nodes, columns),
        out_shape=jax.ShapeDtypeStruct((tok_dev, D), jnp.bfloat16),
        in_specs=[vmem, anywhere, vmem, vmem, vmem, anywhere, anywhere],
        out_specs=vmem,
        scratch_shapes=[
            pltpu.VMEM((D, hidden_units), jnp.bfloat16),
            pltpu.VMEM((hidden_units, D), jnp.bfloat16),
            pltpu.VMEM((tok_dev, D), jnp.float32),
            pltpu.VMEM((cells, D), jnp.float32),
            pltpu.VMEM((2, cells, WIDE), jnp.bfloat16),
            pltpu.VMEM((tok_dev, D), jnp.float32),
            packed,
            guides,
            packed,
            guides,
            grouped,
            grouped,
            grouped,
            grouped,
            packed,
            packed,
            pltpu.SemaphoreType.DMA((3,)),
        ]
        + [hop_sems] * 6
        + [peer_sems] * 4,
        compiler_params=pltpu.CompilerParams(
            collective_id=2, has_side_effects=True, vmem_limit_bytes=62 * 1024 * 1024
        ),
    )(
        normed,
        hidden,
        gate,
        expert.reshape(1, tok_dev),
        slot.reshape(1, tok_dev),
        w_up,
        w_down,
    )


def exchange_by_blocks(outgoing, w_up, w_down):
    experts, cap, _ = outgoing.shape
    block = lax.all_to_all(
        outgoing.reshape(experts, 1, cap, D),
        ("node", "expert"),
        split_axis=0,
        concat_axis=1,
        tiled=True,
    )
    token_rows = block.reshape(-1, D)
    lifted = jnp.dot(token_rows, w_up[0], preferred_element_type=jnp.float32)
    lifted = jax.nn.gelu(lifted, approximate=True).astype(jnp.bfloat16)
    result = jnp.dot(lifted, w_down[0], preferred_element_type=jnp.float32).astype(jnp.bfloat16)
    return lax.all_to_all(
        result.reshape(block.shape), ("node", "expert"), split_axis=1, concat_axis=0, tiled=True
    )


def shards(
    tokens,
    queries,
    keys,
    values,
    neighbours,
    live_bits,
    out_proj,
    norm_gain,
    router,
    expert,
    slot,
    w_up,
    w_down,
):
    tok_dev = tokens.shape[0]
    experts = router.shape[1]
    cap = 2 * tok_dev // experts
    hidden, normed, gate, level = attention_block(
        tokens, queries, keys, values, neighbours, live_bits, out_proj, norm_gain, router, expert
    )

    def padded_way():
        slot_cell = expert * cap + slot
        one_hot = (lax.iota(jnp.int32, experts * cap)[:, None] == slot_cell[None, :]).astype(
            jnp.bfloat16
        )
        outgoing = jnp.dot(one_hot, normed, preferred_element_type=jnp.float32).astype(
            jnp.bfloat16
        )
        exchange = exchange_by_blocks if cap % 16 else expert_exchange
        returned = exchange(outgoing.reshape(experts, cap, D), w_up, w_down)
        flat_back = returned.reshape(experts * cap, D)
        expert_out = jnp.einsum(
            "ct,cd->td", one_hot, flat_back, preferred_element_type=jnp.float32
        )
        layer_out = hidden + gate[:, :1] * expert_out
        return layer_out.astype(jnp.bfloat16)

    def relayed_way():
        return relay_exchange(fit, normed, hidden, gate, expert, slot, w_up, w_down)

    fit = 2 * tok_dev // GROUPS * 3 // 4
    if cap % 16 or lax.axis_size("node") % GROUPS:
        return padded_way()
    return lax.cond(level[0, 0] <= fit, relayed_way, padded_way)


def solution(mesh):
    in_specs = (
        P(("node", "expert"), None),
        P(("node", "expert"), None),
        P(("node", "expert"), None),
        P(("node", "expert"), None),
        P(("node", "expert"), None),
        P(("node", "expert"), None),
        P(),
        P(),
        P(),
        P(("node", "expert")),
        P(("node", "expert")),
        P(("node", "expert"), None, None),
        P(("node", "expert"), None, None),
    )
    out_specs = P(("node", "expert"), None)
    return jax.shard_map(shards, mesh=mesh, in_specs=in_specs, out_specs=out_specs, check_vma=False)
```
